128 devices in a mesh: expert: 32 (over y, x, core), dp: 4 (over z).
Axes of the slice: x: 4, y: 4, z: 4, core: 2. Of those that a mesh axis runs over, the one named last changes fastest.
Arguments:
- out_grads: bfloat16 [4, 4096, 7168], P('dp', 'expert'), may hold values from -6 to 6
- expert_ids: int32 [4, 4096, 8], P('dp', 'expert'), may hold values from 0 to 255, all different within a row; in each aligned block of 128 rows (0 to 127, 128 to 255, ..., all dimensions but the last counted through in order) at most 6 rows name the same one
- gate_probs: float32 [4, 4096, 8], P('dp', 'expert'), may hold values from 0.05 to 0.5
- hidden_acts: bfloat16 [4, 256, 192, 2048], P('dp', 'expert'), may hold values from -6 to 6
- q_previous: bfloat16 [256, 32, 7168], P('expert'), may hold values from -0.0625 to 0.0625
Outputs:
- new_basis: float32 [256, 32, 2048], P('expert')
- q_update: float32 [256, 32, 7168], P('expert', None, 'dp')
The draws below stay inside these ranges and needn't reach their ends.
Inputs may be any that keep to these rules, and one draw needn't show every extreme that they name: `expert_ids`: each row names 8 different experts; among the rows of one device no expert is named more than 6 times.
All inputs are finite; a program needn't handle non-finite values.
Results may differ from the reference program's by a relative error of at most 0.014.
Values may be sent and summed in bfloat16 or wider, within the bound.
A program may use at most 192 MiB of HBM per device.

```python
import math
import jax
import jax.numpy as jnp
import numpy as np
from jax import lax

D = 7168
FF = 2048
TOP = 8
RANK = 32
TOK_DEV = 128
EXPERTS = 256
CAP = 6
SLOTS = 192
TOK_EXP = 4096
N_EXPERT = 32
N_DP = 4


def steps_of(key, extent, shards, smallest, top_value):
    factor_of, own = 1.0, jax.random.fold_in(key, 6)
    for dim, parts in shards:
        heights = jnp.exp(jax.random.uniform(jax.random.fold_in(own, dim), (parts,), jnp.float32, smallest / len(shards), top_value / len(shards)))
        factor_of = factor_of * jnp.repeat(heights, extent[dim] // parts).reshape([-1 if axis == dim else 1 for axis in range(len(extent))])
    return factor_of


def routed_block(rng, own, number, rows, count, top, limit, skew):
    ranking = jax.random.permutation(rng, count)
    crowded, usual = portions_of(count, rows * top, limit, skew, True), portions_of(count, rows * top, limit, skew, False)
    places = jnp.arange(count)

    def named(tallies, rotation):
        used = int((tallies > 0).sum())
        fixed = max(1, used // 4)
        passed = fixed + (places - fixed + rotation * (used - fixed)) % max(1, count - fixed)
        return jnp.zeros((count,), jnp.int32).at[ranking[jnp.where(places < fixed, places, passed)]].set(jnp.asarray(tallies, jnp.int32))

    tallies = jnp.where(number % 4 == 0, named(crowded, number // 4), named(usual, number - number // 4 - 1))
    mixed = jax.random.permutation(jax.random.fold_in(own, 3), count)
    source_of, sink = mixed[0:count // 2 * 2:2], mixed[1:count // 2 * 2:2]
    room = jnp.minimum(tallies[source_of] - 1, limit - tallies[sink]) // 2
    room = jnp.where((source_of == ranking[0]) | (sink == ranking[0]) | (tallies[sink] == 0), 0, jnp.maximum(room, 0))
    passed = jax.random.randint(jax.random.fold_in(own, 4), (count // 2,), 0, 1 << 20) % (room + 1)
    tallies = tallies.at[source_of].add(-passed).at[sink].add(passed)
    labels = jnp.searchsorted(jnp.cumsum(tallies), jnp.arange(rows * top), side="right").astype(jnp.int32)
    grid = labels.reshape(top, rows).T
    grid = grid[jax.random.permutation(jax.random.fold_in(own, 1), rows)]
    rotation = jax.random.randint(jax.random.fold_in(own, 2), (rows, 1), 0, top)
    return jnp.take_along_axis(grid, (jnp.arange(top)[None, :] + rotation) % top, axis=1)


def portions_of(number_of, total, bound, slope, full):
    weights = [(1 << 20) // math.isqrt(grade ** slope) + 1 for grade in range(1, number_of + 1)]
    largest = bound if full else min(bound, max(-(-total // number_of), total * weights[0] // sum(weights)))
    least = 1 if total - largest >= number_of - 1 else 0
    given, surplus = [largest] + [least] * (number_of - 1), total - largest - least * (number_of - 1)
    while surplus > 0:
        free = [i for i in range(1, number_of) if given[i] < largest] or [i for i in range(1, number_of) if given[i] < bound]
        mass, budget = sum([weights[i] for i in free]), surplus
        for i in free:
            more = min(bound - given[i], max(1, budget * weights[i] // mass), surplus)
            given[i] = given[i] + more
            surplus = surplus - more
    return np.array(given)


def noise(key, shape, deviation, bound, cuts=(), kind=jnp.bfloat16):
    factor_of = steps_of(key, shape, cuts, -0.22, 0.18) if cuts else 1.0
    result = jax.random.normal(key, shape, jnp.float32) * deviation * factor_of
    return jnp.minimum(jnp.maximum(result, -bound), bound).astype(kind)


def setup_inputs(seed: int = 0) -> dict:
    arg_keys = jax.random.split(jax.random.key(seed), 6)
    out_grads = noise(arg_keys[0], (N_DP, TOK_EXP, D), 1.0, 6.0, ((0, 4), (1, 32)))
    expert_ids_keys = jax.random.split(jax.random.fold_in(arg_keys[1], 1), N_DP * TOK_EXP // TOK_DEV)
    expert_ids_turns = jax.random.permutation(jax.random.fold_in(arg_keys[1], 3), N_DP * TOK_EXP // TOK_DEV)
    expert_ids = jax.vmap(lambda own, number: routed_block(jax.random.fold_in(arg_keys[1], 2), own, number, TOK_DEV, EXPERTS, TOP, CAP, 1))(expert_ids_keys, expert_ids_turns).reshape((N_DP, TOK_EXP, TOP))
    gate_probs = jnp.clip(0.05 + 0.45 * jax.random.uniform(arg_keys[2], (N_DP, TOK_EXP, TOP), jnp.float32) ** steps_of(arg_keys[2], (N_DP, TOK_EXP, TOP), ((0, 4), (1, 32)), -0.2, 0.2), 0.05, 0.5)
    hidden_acts = noise(arg_keys[3], (N_DP, EXPERTS, SLOTS, FF), 1.0, 6.0, ((0, 4), (1, 32)))
    q_previous = noise(arg_keys[4], (EXPERTS, RANK, D), D ** -0.5, 0.0625, ((0, 32),))
    return {"out_grads": out_grads, "expert_ids": expert_ids, "gate_probs": gate_probs, "hidden_acts": hidden_acts, "q_previous": q_previous}


def to_half(values):
    return lax.optimization_barrier(values.astype(jnp.bfloat16))

def slot_tables(route_ids, gate_values, num_experts, capacity):
    flat_ids = route_ids.reshape(-1)
    row_count = flat_ids.shape[0]
    top_k = route_ids.shape[-1]
    one_hot = (flat_ids[:, None] == jnp.arange(num_experts, dtype=jnp.int32)[None, :]).astype(jnp.int32)
    earlier = jnp.cumsum(one_hot, axis=0) - one_hot
    position = lax.optimization_barrier(jnp.sum(earlier * one_hot, axis=1)).astype(jnp.int32)
    slot_index = (flat_ids * capacity + position).astype(jnp.int32)
    token_of = jnp.zeros((num_experts * capacity,), jnp.int32).at[slot_index].set((jnp.arange(row_count, dtype=jnp.int32) // top_k).astype(jnp.int32))
    gate_of = jnp.zeros((num_experts * capacity,), jnp.float32).at[slot_index].set(gate_values.reshape(-1).astype(jnp.float32))
    return (token_of, gate_of)

def reference(out_grads, expert_ids, gate_probs, hidden_acts, q_previous):
    grads_blocks = out_grads.reshape(N_DP, N_EXPERT, TOK_DEV, D)
    id_blocks = expert_ids.reshape(N_DP, N_EXPERT, TOK_DEV, TOP)
    gate_blocks = gate_probs.reshape(N_DP, N_EXPERT, TOK_DEV, TOP)
    tables = jax.vmap(jax.vmap(lambda ids, gts: slot_tables(ids, gts, EXPERTS, CAP)))
    token_of, gate_of = tables(id_blocks, gate_blocks)

    def pick_rows(grads_one, tokens_one):
        return jnp.take(grads_one, tokens_one, axis=0)

    def one_expert(expert_num):
        start = (expert_num * CAP).astype(jnp.int32)
        tokens_here = lax.dynamic_slice_in_dim(token_of, start, CAP, 2)
        gates_here = lax.dynamic_slice_in_dim(gate_of, start, CAP, 2)
        picked = jax.vmap(jax.vmap(pick_rows))(grads_blocks, tokens_here)
        routed = to_half(picked.astype(jnp.float32) * gates_here[..., None]).reshape(N_DP, SLOTS, D)
        hidden_here = lax.dynamic_index_in_dim(hidden_acts, expert_num, 1, keepdims=False)
        q_here = lax.dynamic_index_in_dim(q_previous, expert_num, 0, keepdims=False)
        mixed = to_half(jnp.einsum('psd,rd->psr', routed.astype(jnp.float32), q_here.astype(jnp.float32)))
        factor = jnp.einsum('psr,psf->rf', mixed.astype(jnp.float32), hidden_here.astype(jnp.float32))
        gram = jnp.dot(factor, factor.T, precision=lax.Precision.HIGHEST)
        lower = jnp.linalg.cholesky(gram)
        inverse = jax.scipy.linalg.solve_triangular(lower, jnp.eye(RANK, dtype=jnp.float32), lower=True)
        ortho = jnp.dot(inverse, factor, precision=lax.Precision.HIGHEST)
        ortho_half = to_half(ortho)
        projected = to_half(jnp.einsum('psf,rf->psr', hidden_here.astype(jnp.float32), ortho_half.astype(jnp.float32)))
        q_new = jnp.einsum('psr,psd->rd', projected.astype(jnp.float32), routed.astype(jnp.float32))
        return (ortho * math.sqrt(FF), q_new)
    new_basis, q_update = lax.map(one_expert, jnp.arange(EXPERTS, dtype=jnp.int32))
    return (new_basis, q_update)
```

```python
import math

import jax
import jax.numpy as jnp
from jax import lax
from jax.experimental import pallas as pl
from jax.experimental.pallas import tpu as pltpu
from jax.sharding import PartitionSpec as P

MESH = pl.DeviceIdType.MESH
BF, F32 = jnp.bfloat16, jnp.float32
HI = lax.Precision.HIGHEST
SLOT = 8
CAP = 6


def dot_nt(left, right, **more):
    return lax.dot_general(left, right, (((1,), (1,)), ((), ())), preferred_element_type=F32, **more)


def dot_nn(left, right, **more):
    return lax.dot_general(left, right, (((1,), (0,)), ((), ())), preferred_element_type=F32, **more)


def dot_tn(left, right, **more):
    return lax.dot_general(left, right, (((0,), (0,)), ((), ())), preferred_element_type=F32, **more)


def iota(shape, dim):
    return lax.broadcasted_iota(jnp.int32, shape, dim)


def slot_selection():
    row, slot = iota((256, 192), 0), iota((256, 192), 1)
    x, y, core, place = row // 64, (row // 16) % 4, (row // 8) % 2, row % 8
    at = ((y * 4 + x) * 2 + core) * CAP + place
    return jnp.where((at == slot) & (place < CAP), 1.0, 0.0).astype(BF)


def kernel(
    ids_ref, gates_ref, grads_ref, hidden_ref, prev_ref, basis_ref, update_ref,
    tok, meta, q_row, routed, pick, gate_col, hid, m_out, m_in, m_t, f_out, f_in, fac, orth, p_out, p_in,
    load_sem, zs, zr, as_, ar, hs, hr, ps, pr,
    mzs, mzr, mas, mar, mhs, mhr, mps, mpr,
    qs, qr, ms, mr, fs, fr, os_, or_, js, jr, us, ur,
):
    width = tok.shape[2]
    e, z = lax.axis_index("expert"), lax.axis_index("dp")
    y, x, c = e // 8, (e // 2) % 4, e % 2

    def dev(yy, xx, cc, zz):
        return {"expert": (yy * 4 + xx) * 2 + cc, "dp": zz}

    def turn(v, by):
        return lax.rem(v + by, 4)

    def copy(src, dst, send, recv, device):
        return pltpu.make_async_remote_copy(src, dst, send, recv, device_id=device, device_id_type=MESH)

    def block(zz, yy, cc):
        return (zz * 4 + yy) * 2 + cc

    cols = lambda zz: pl.ds(pl.multiple_of(zz * width, 128), width)

    own = block(z, y, c)
    load_tok = pltpu.make_async_copy(grads_ref.at[:, cols(z)], tok.at[own], load_sem.at[0])
    load_q = pltpu.make_async_copy(prev_ref.at[:, cols(z)], q_row.at[x], load_sem.at[1])
    load_hid = pltpu.make_async_copy(hidden_ref, hid, load_sem.at[2])
    load_tok.start()
    load_q.start()
    load_hid.start()

    barrier = pltpu.get_barrier_semaphore()
    peers = [dev(turn(y, 1), x, c, z), dev(turn(y, 3), x, c, z), dev(y, x, 1 - c, z)]
    for bx in range(4):
        for bz in range(4):
            if bx or bz:
                peers.append(dev(y, turn(x, bx), c, turn(z, bz)))
    for peer in peers:
        pl.semaphore_signal(barrier, inc=1, device_id=peer, device_id_type=MESH)

    ids = ids_ref[...]
    expert_row = iota((256, 128), 0)
    named = jnp.zeros((256, 128), F32)
    for k in range(8):
        named = named + jnp.where(ids[k : k + 1, :] == expert_row, 1.0, 0.0)
    before = jnp.where(iota((128, 128), 0) < iota((128, 128), 1), 1.0, 0.0).astype(BF)
    earlier = dot_nn(named.astype(BF), before)
    place = jnp.concatenate(
        [
            jnp.sum(jnp.where(ids[k : k + 1, :] == expert_row, earlier, 0.0), axis=0, keepdims=True)
            for k in range(8)
        ],
        axis=0,
    )
    holder, inner = ids // 8, ids % 8
    group = (holder // 8) * 2 + holder % 2
    base = group * 512 + ((holder // 2) % 4) * 128 + inner * 16
    meta[own, 0:8, :] = base.astype(F32) + place
    meta[own, 8:16, :] = gates_ref[...]

    pl.semaphore_wait(barrier, len(peers))

    waits = []

    def go(cp):
        cp.start()
        waits.append(cp)

    zorder = [0, 1, 3, 2]
    for r in (1, 3, 2):
        to = turn(z, r)
        go(copy(meta.at[own], meta.at[own], mzs.at[r], mzr.at[r], dev(y, x, c, to)))
        go(copy(grads_ref.at[:, cols(to)], tok.at[own], zs.at[r], zr.at[r], dev(y, x, c, to)))
    load_q.wait()
    for r in (2, 1, 3):
        go(copy(q_row.at[x], q_row.at[x], qs.at[r], qr.at[r], dev(y, turn(x, r), c, z)))
    load_tok.wait()

    up, down, partner = dev(turn(y, 1), x, c, z), dev(turn(y, 3), x, c, z), dev(y, x, 1 - c, z)

    def to_partner(k, zz, dy):
        b = block(zz, turn(y, dy), c)
        go(copy(meta.at[b], meta.at[b], mps.at[k, dy], mpr.at[k, dy], partner))
        go(copy(tok.at[b], tok.at[b], ps.at[k, dy], pr.at[k, dy], partner))

    def source(k):
        return turn(z, zorder[k])

    def stage_a(k):
        zz = source(k)
        b = block(zz, y, c)
        if k:
            r = (4 - zorder[k]) % 4
            copy(meta.at[b], meta.at[b], mzs.at[r], mzr.at[r], up).wait_recv()
            copy(tok.at[b], tok.at[b], zs.at[r], zr.at[r], up).wait_recv()
        for way, device in ((0, up), (1, down)):
            go(copy(meta.at[b], meta.at[b], mas.at[way, k], mar.at[way, k], device))
            go(copy(tok.at[b], tok.at[b], as_.at[way, k], ar.at[way, k], device))
        to_partner(k, zz, 0)

    def stage_b(k):
        zz = source(k)
        for way, device, dy in ((0, up, 3), (1, down, 1)):
            b = block(zz, turn(y, dy), c)
            copy(meta.at[b], meta.at[b], mas.at[way, k], mar.at[way, k], device).wait_recv()
            copy(tok.at[b], tok.at[b], as_.at[way, k], ar.at[way, k], device).wait_recv()
            half = pl.ds(way * 64, 64)
            if way == 0:
                go(copy(meta.at[b], meta.at[b], mhs.at[k], mhr.at[k], device))
            go(copy(tok.at[b, half], tok.at[b, half], hs.at[way, k], hr.at[way, k], device))
            to_partner(k, zz, dy)

    def stage_h(k):
        zz = source(k)
        b = block(zz, turn(y, 2), c)
        copy(meta.at[b], meta.at[b], mhs.at[k], mhr.at[k], up).wait_recv()
        for way in range(2):
            half = pl.ds(way * 64, 64)
            copy(tok.at[b, half], tok.at[b, half], hs.at[way, k], hr.at[way, k], up).wait_recv()
        to_partner(k, zz, 2)

    mine = ((y * 2 + c) * 512).astype(F32)
    row_of = iota((512, 128), 0).astype(F32)

    def rows_of(zz, yy):
        pair = zz * 4 + yy
        gates = []
        for cc in range(2):
            info = meta[pair * 2 + cc]
            want = info[0:8] - mine + float(cc * 8)
            gate = jnp.zeros((512, 128), F32)
            for k in range(8):
                gate = jnp.where(row_of == want[k : k + 1], info[8 + k : 9 + k], gate)
            gates.append(gate)
            pick[:, cc * 128 : cc * 128 + 128] = jnp.where(gate > 0.0, 1.0, 0.0).astype(BF)
        gate_col[...] = jnp.broadcast_to(
            jnp.sum(gates[0] + gates[1], axis=1, keepdims=True), gate_col.shape
        )
        to = pl.ds(pl.multiple_of(pair * 16, 16), 16)

        @pl.loop(0, width // 256)
        def _(n):
            at = pl.ds(pl.multiple_of(n * 256, 256), 256)
            rows = jnp.concatenate([tok[pair * 2, :, at], tok[pair * 2 + 1, :, at]], axis=0)
            got = dot_nn(pick[...], rows)
            gate = gate_col[...]
            got = got * jnp.concatenate([gate, gate], axis=1)
            routed[:, to, at] = got.astype(BF).reshape(32, 16, 256)

    lane_expert = iota((64, 256), 1) // 32

    def stage_c(k):
        zz = source(k)
        for dy in range(4):
            b = block(zz, turn(y, dy), 1 - c)
            copy(meta.at[b], meta.at[b], mps.at[k, dy], mpr.at[k, dy], partner).wait_recv()
            copy(tok.at[b], tok.at[b], ps.at[k, dy], pr.at[k, dy], partner).wait_recv()

        @pl.loop(0, 4)
        def _(i):
            rows_of(zz, i)

        part = pl.ds(pl.multiple_of(zz * 64, 64), 64)
        if k == 0:
            for r in (1, 2, 3):
                b = turn(x, 4 - r)
                copy(q_row.at[b], q_row.at[b], qs.at[r], qr.at[r], up).wait_recv()
        for r in range(4):
            to = turn(x, r)
            rows = routed[pl.ds(to * 8, 8), part, :].reshape(512, width)
            every = dot_nt(rows, q_row[to])
            total = jnp.zeros((64, 256), F32)
            for j in range(8):
                total = total + jnp.where(lane_expert == j, every[j * 64 : j * 64 + 64], 0.0)
            if k == 0 and r == 0:
                m_in[0, 0] = total.astype(BF)
            else:
                m_out[k, r] = total.astype(BF)
                go(
                    copy(
                        m_out.at[k, r],
                        m_in.at[r, k],
                        ms.at[k, r],
                        mr.at[k, r],
                        dev(y, to, c, zz),
                    )
                )

    stage_a(0)
    stage_a(1)
    stage_b(0)
    stage_a(2)
    stage_h(0)
    stage_b(1)
    stage_c(0)
    stage_a(3)
    stage_h(1)
    stage_b(2)
    stage_c(1)
    stage_h(2)
    stage_b(3)
    stage_c(2)
    stage_h(3)
    stage_c(3)

    while waits:
        waits.pop(0).wait_send()

    load_hid.wait()
    parts = []
    for r in range(4):
        total = None
        for k in range(4):
            if k or r:
                copy(m_out.at[k, r], m_in.at[r, k], ms.at[k, r], mr.at[k, r], up).wait_recv()
            got = m_in[r, k].astype(F32)
            total = got if total is None else total + got
        parts.append(total.astype(BF))
    raw = jnp.concatenate(parts, axis=0)

    def selection():
        row, slot = iota((256, 192), 0), iota((256, 192), 1)
        from_x = (x + 4 - row // 64) % 4
        at = ((((row // 16) % 4) * 4 + from_x) * 2 + (row // 8) % 2) * CAP + row % 8
        return jnp.where((at == slot) & (row % 8 < CAP), 1.0, 0.0).astype(BF)

    select = selection()
    m_t[...] = dot_tn(raw, select).astype(BF)

    for k, r in enumerate((2, 1, 3, 0)):
        to = turn(z, r)
        for i in range(2):
            j = to * 2 + i
            rows = m_t[pl.ds(pl.multiple_of(j * 32, 32), 32), :]
            got = dot_nn(rows, hid[j])
            if r:
                f_out[r, i * 32 : i * 32 + 32, :] = got.astype(BF)
            else:
                fac[i * 32 : i * 32 + 32, :] = got
        if r:
            go(copy(f_out.at[r], f_in.at[r], fs.at[r], fr.at[r], dev(y, x, c, to)))
    total = fac[0:64, :]
    for r in (1, 3, 2):
        copy(f_out.at[r], f_in.at[r], fs.at[r], fr.at[r], up).wait_recv()
        total = total + f_in[r].astype(F32)
    fac[0:64, :] = total
    fac[64:128, :] = total

    gram = dot_nt(fac[0:64, :], fac[...], precision=HI)
    lane, row = iota((32, 128), 1), iota((32, 128), 0)
    eye = jnp.where(lane % 32 == row, 1.0, 0.0)
    work = jnp.where(lane >= 96, gram[32:64], jnp.where(lane >= 64, gram[0:32], eye))
    first = (lane // 32) % 2 == 0
    for k in range(32):
        one = jnp.sum(jnp.where(lane == 64 + k, work, 0.0), axis=1, keepdims=True)
        two = jnp.sum(jnp.where(lane == 96 + k, work, 0.0), axis=1, keepdims=True)
        one = one / one[k : k + 1, :]
        two = two / two[k : k + 1, :]
        factor = jnp.where(row > k, jnp.where(first, one, two), 0.0)
        work = work - factor * work[k : k + 1, :]
    one = jnp.sum(jnp.where(lane == 64 + row, work, 0.0), axis=1, keepdims=True)
    two = jnp.sum(jnp.where(lane == 96 + row, work, 0.0), axis=1, keepdims=True)
    work = work * jnp.where(first, 1.0 / jnp.sqrt(one), 1.0 / jnp.sqrt(two))
    inverse = jnp.concatenate(
        [jnp.where(lane < 32, work, 0.0), jnp.where((lane >= 32) & (lane < 64), work, 0.0)], axis=0
    )
    ortho = dot_nn(inverse[:, 0:64], fac[0:64, :], precision=HI)
    orth[z] = ortho.astype(BF)
    for r in (2, 1, 3):
        go(copy(orth.at[z], orth.at[z], os_.at[r], or_.at[r], dev(y, x, c, turn(z, r))))

    root = math.sqrt(hid.shape[2])
    for r in (0, 1, 3, 2):
        zz = turn(z, 4 - r)
        if r:
            copy(orth.at[zz], orth.at[zz], os_.at[r], or_.at[r], up).wait_recv()
        for i in range(2):
            j = zz * 2 + i
            got = dot_nt(orth[zz, i * 32 : i * 32 + 32, :], hid[j])
            m_t[pl.ds(pl.multiple_of(j * 32, 32), 32), :] = got.astype(BF)
    spread = dot_nt(select, m_t[...]).astype(BF)
    for r in range(4):
        p_out[r] = spread[r * 64 : r * 64 + 64]
    for r in (2, 1, 3, 0):
        for q in (2, 1, 3, 0):
            if r or q:
                go(
                    copy(
                        p_out.at[r],
                        p_in.at[r, z],
                        js.at[r, q],
                        jr.at[r, q],
                        dev(y, turn(x, 4 - r), c, turn(z, q)),
                    )
                )
    p_in[0, z] = spread[0:64]
    for zz in range(4):
        basis_ref[zz * 64 : zz * 64 + 64, :] = orth[zz].astype(F32) * root

    for r in (2, 1, 3, 0):
        b = turn(x, r)
        for q in range(4):
            if r or q:
                zz = turn(z, 4 - q)
                copy(p_out.at[r], p_in.at[r, zz], js.at[r, q], jr.at[r, q], up).wait_recv()
        terms = jnp.concatenate([p_in[r, zz] for zz in range(4)], axis=0)
        pick[0:256, :] = terms.astype(F32).T.astype(BF)

        @pl.loop(0, 8)
        def _(j):
            at = pl.ds(pl.multiple_of(j * 32, 32), 32)
            got = dot_nn(pick[at, :], routed[b * 8 + j])
            if r:
                to = pl.ds(pl.multiple_of((j % 4) * 32, 32), 32)
                tok[2 * r + j // 4, to, :] = got.astype(BF)
            else:
                update_ref[at, :] = got

        if r:
            go(
                copy(
                    tok.at[pl.ds(2 * r, 2)],
                    tok.at[pl.ds(8 + 2 * r, 2)],
                    us.at[r],
                    ur.at[r],
                    dev(y, b, c, z),
                )
            )
    for r in (1, 3, 2):
        copy(tok.at[pl.ds(2 * r, 2)], tok.at[pl.ds(8 + 2 * r, 2)], us.at[r], ur.at[r], up).wait_recv()

        @pl.loop(0, 8)
        def _(j):
            at = pl.ds(pl.multiple_of(j * 32, 32), 32)
            to = pl.ds(pl.multiple_of((j % 4) * 32, 32), 32)
            update_ref[at, :] = update_ref[at, :] + tok[8 + 2 * r + j // 4, to, :].astype(F32)

    for cp in waits:
        cp.wait_send()


def local(out_grads, expert_ids, gate_probs, hidden_acts, q_previous):
    experts, rank, model = q_previous.shape
    hidden_units = hidden_acts.shape[3]
    width = model // lax.axis_size("dp")
    any_spec, vmem = pl.BlockSpec(memory_space=pl.ANY), pl.BlockSpec(memory_space=pltpu.VMEM)
    dma = lambda *shape: pltpu.SemaphoreType.DMA(shape)
    basis, update = pl.pallas_call(
        kernel,
        out_shape=(
            jax.ShapeDtypeStruct((experts * rank, hidden_units), F32),
            jax.ShapeDtypeStruct((experts * rank, width), F32),
        ),
        in_specs=[vmem, vmem, any_spec, any_spec, any_spec],
        out_specs=(vmem, vmem),
        scratch_shapes=[
            pltpu.VMEM((32, 128, width), BF),
            pltpu.VMEM((32, 16, 128), F32),
            pltpu.VMEM((4, 256, width), BF),
            pltpu.VMEM((32, 256, width), BF),
            pltpu.VMEM((512, 256), BF),
            pltpu.VMEM((512, 128), F32),
            pltpu.VMEM((8, 192, hidden_units), BF),
            pltpu.VMEM((4, 4, 64, 256), BF),
            pltpu.VMEM((4, 4, 64, 256), BF),
            pltpu.VMEM((256, 192), BF),
            pltpu.VMEM((4, 64, hidden_units), BF),
            pltpu.VMEM((4, 64, hidden_units), BF),
            pltpu.VMEM((128, hidden_units), F32),
            pltpu.VMEM((4, 64, hidden_units), BF),
            pltpu.VMEM((4, 64, 256), BF),
            pltpu.VMEM((4, 4, 64, 256), BF),
            dma(3),
            dma(4), dma(4), dma(2, 4), dma(2, 4), dma(2, 4), dma(2, 4), dma(4, 4), dma(4, 4),
            dma(4), dma(4), dma(2, 4), dma(2, 4), dma(4), dma(4), dma(4, 4), dma(4, 4),
            dma(4), dma(4), dma(4, 4), dma(4, 4), dma(4), dma(4), dma(4), dma(4),
            dma(4, 4), dma(4, 4), dma(4), dma(4),
        ],
        compiler_params=pltpu.CompilerParams(
            collective_id=0, has_side_effects=True, vmem_limit_bytes=67043328
        ),
    )(
        expert_ids[0].T,
        gate_probs[0].T,
        out_grads[0],
        hidden_acts[0],
        q_previous.reshape(experts * rank, model),
    )
    return (basis.reshape(experts, rank, hidden_units), update.reshape(experts, rank, width))


def solution(mesh):
    return jax.shard_map(
        local,
        mesh=mesh,
        in_specs=(
            P("dp", "expert", None),
            P("dp", "expert", None),
            P("dp", "expert", None),
            P("dp", "expert", None, None),
            P("expert", None, None),
        ),
        out_specs=(P("expert", None, None), P("expert", None, "dp")),
        check_vma=False,
    )
```

```python
import math

import jax
import jax.numpy as jnp
from jax import lax
from jax.experimental import pallas as pl
from jax.experimental.pallas import tpu as pltpu
from jax.sharding import PartitionSpec as P

MESH = pl.DeviceIdType.MESH
BF, F32 = jnp.bfloat16, jnp.float32
HI = lax.Precision.HIGHEST
SLOT = 8
CAP = 6


def dot_nt(left, right, **more):
    return lax.dot_general(left, right, (((1,), (1,)), ((), ())), preferred_element_type=F32, **more)


def dot_nn(left, right, **more):
    return lax.dot_general(left, right, (((1,), (0,)), ((), ())), preferred_element_type=F32, **more)


def dot_tn(left, right, **more):
    return lax.dot_general(left, right, (((0,), (0,)), ((), ())), preferred_element_type=F32, **more)


def iota(shape, dim):
    return lax.broadcasted_iota(jnp.int32, shape, dim)


def kernel(
    ids_ref, gates_ref, grads_ref, hidden_ref, prev_ref, basis_ref, update_ref,
    tok, meta, q_row, routed, hid, m_out, m_in, m_t, hf, f_out, f_in, f_own, f_all, low, p_in, p_t,
    load_sem, zs, zr, as_, ar, hs, hr, ps, pr,
    mzs, mzr, mas, mar, mhs, mhr, mps, mpr,
    qs, qr, ms, mr, fs, fr, gs, gr, ls, lr, js, jr, us, ur,
):
    width = tok.shape[3]
    e, z = lax.axis_index("expert"), lax.axis_index("dp")
    y, x, c = e // 8, (e // 2) % 4, e % 2
    gather, spread = (y, x), (x, y)

    def turn(v, by):
        return lax.rem(v + by, 4)

    def dev(h, along_gather, along_spread, to_z, core=0):
        g, s = turn(gather[h], along_gather), turn(spread[h], along_spread)
        yy, xx = (g, s) if h == 0 else (s, g)
        cc = 1 - c if core else c
        return {"expert": (yy * 4 + xx) * 2 + cc, "dp": turn(z, to_z)}

    def copy(src, dst, send, recv, device):
        return pltpu.make_async_remote_copy(src, dst, send, recv, device_id=device, device_id_type=MESH)

    def block(zz, gg, cc):
        return (zz * 4 + gg) * 2 + cc

    def cols(zz, h):
        return pl.ds(pl.multiple_of(zz * (2 * width) + h * width, 128), width)

    own = [block(z, gather[h], c) for h in range(2)]
    load_tok = [
        pltpu.make_async_copy(grads_ref.at[:, cols(z, h)], tok.at[h, own[h]], load_sem.at[h])
        for h in range(2)
    ]
    load_q = [
        pltpu.make_async_copy(prev_ref.at[:, cols(z, h)], q_row.at[h, spread[h]], load_sem.at[2 + h])
        for h in range(2)
    ]
    load_hid = pltpu.make_async_copy(hidden_ref, hid, load_sem.at[4])
    for cp in load_tok + load_q + [load_hid]:
        cp.start()

    barrier = pltpu.get_barrier_semaphore()
    peers = [dev(0, 0, 0, 0, core=1)] + [dev(0, 0, 0, r) for r in (1, 2, 3)]
    for h in range(2):
        for b in (1, 2, 3):
            for r in range(4):
                peers.append(dev(h, 0, b, r))
    for peer in peers:
        pl.semaphore_signal(barrier, inc=1, device_id=peer, device_id_type=MESH)

    ids = ids_ref[...]
    expert_row = iota((256, 128), 0)
    named = jnp.zeros((256, 128), F32)
    for k in range(8):
        named = named + jnp.where(ids[k : k + 1, :] == expert_row, 1.0, 0.0)
    before = jnp.where(iota((128, 128), 0) < iota((128, 128), 1), 1.0, 0.0).astype(BF)
    earlier = dot_nn(named.astype(BF), before)
    place = jnp.concatenate(
        [
            jnp.sum(jnp.where(ids[k : k + 1, :] == expert_row, earlier, 0.0), axis=0, keepdims=True)
            for k in range(8)
        ],
        axis=0,
    )
    holder, inner = ids // 8, ids % 8
    at_y, at_x, at_c = holder // 8, (holder // 2) % 4, holder % 2
    for h, (g, s) in enumerate(((at_y, at_x), (at_x, at_y))):
        base = (g * 2 + at_c) * 256 + (s * 8 + inner) * SLOT
        meta[h, own[h], 0:8, :] = base.astype(F32) + place
        meta[h, own[h], 8:16, :] = gates_ref[...]

    pl.semaphore_wait(barrier, len(peers))

    waits = []

    def go(cp):
        cp.start()
        waits.append(cp)

    zorder = [0, 1, 3, 2]
    for r in (1, 3, 2):
        for h in range(2):
            b = own[h]
            to = turn(z, r)
            go(copy(meta.at[h, b], meta.at[h, b], mzs.at[h, r], mzr.at[h, r], dev(0, 0, 0, r)))
            go(copy(grads_ref.at[:, cols(to, h)], tok.at[h, b], zs.at[h, r], zr.at[h, r], dev(0, 0, 0, r)))

    partner = dev(0, 0, 0, 0, core=1)

    def to_partner(h, k, zz, dg):
        b = block(zz, turn(gather[h], dg), c)
        go(copy(meta.at[h, b], meta.at[h, b], mps.at[h, k, dg], mpr.at[h, k, dg], partner))
        go(copy(tok.at[h, b], tok.at[h, b], ps.at[h, k, dg], pr.at[h, k, dg], partner))

    def source(k):
        return turn(z, zorder[k])

    def stage_a(k):
        zz = source(k)
        for h in range(2):
            b = block(zz, gather[h], c)
            if k:
                r = (4 - zorder[k]) % 4
                copy(meta.at[h, b], meta.at[h, b], mzs.at[h, r], mzr.at[h, r], partner).wait_recv()
                copy(tok.at[h, b], tok.at[h, b], zs.at[h, r], zr.at[h, r], partner).wait_recv()
            else:
                load_tok[h].wait()
            for way, step in ((0, 1), (1, 3)):
                device = dev(h, step, 0, 0)
                go(copy(meta.at[h, b], meta.at[h, b], mas.at[h, way, k], mar.at[h, way, k], device))
                go(copy(tok.at[h, b], tok.at[h, b], as_.at[h, way, k], ar.at[h, way, k], device))
            to_partner(h, k, zz, 0)

    def stage_b(k):
        zz = source(k)
        for h in range(2):
            for way, step, dg in ((0, 1, 3), (1, 3, 1)):
                device = dev(h, step, 0, 0)
                b = block(zz, turn(gather[h], dg), c)
                copy(meta.at[h, b], meta.at[h, b], mas.at[h, way, k], mar.at[h, way, k], device).wait_recv()
                copy(tok.at[h, b], tok.at[h, b], as_.at[h, way, k], ar.at[h, way, k], device).wait_recv()
                half = pl.ds(way * 64, 64)
                if way == 0:
                    go(copy(meta.at[h, b], meta.at[h, b], mhs.at[h, k], mhr.at[h, k], device))
                go(copy(tok.at[h, b, half], tok.at[h, b, half], hs.at[h, way, k], hr.at[h, way, k], device))
                to_partner(h, k, zz, dg)

    def stage_h(k):
        zz = source(k)
        for h in range(2):
            b = block(zz, turn(gather[h], 2), c)
            copy(meta.at[h, b], meta.at[h, b], mhs.at[h, k], mhr.at[h, k], partner).wait_recv()
            for way in range(2):
                half = pl.ds(way * 64, 64)
                copy(
                    tok.at[h, b, half], tok.at[h, b, half], hs.at[h, way, k], hr.at[h, way, k], partner
                ).wait_recv()
            to_partner(h, k, zz, 2)

    mine = [((gather[h] * 2 + c) * 256).astype(F32) for h in range(2)]
    row_of = iota((256, 128), 0).astype(F32)
    chunks = [(n, min(256, width - n)) for n in range(0, width, 256)]

    def rows_of(h, zz, gg):
        pair = zz * 4 + gg
        less = jnp.where(h == 0, mine[0], mine[1])
        picks, scales = [], []
        for cc in range(2):
            info = meta[h, pair * 2 + cc]
            want = info[0:8] - less
            gate = jnp.zeros((256, 128), F32)
            for k in range(8):
                gate = jnp.where(row_of == want[k : k + 1], info[8 + k : 9 + k], gate)
            picks.append(jnp.where(gate > 0.0, 1.0, 0.0).astype(BF))
            scales.append(jnp.sum(gate, axis=1, keepdims=True))
        to = pl.ds(pl.multiple_of(pair * 16, 16), 16)
        for n, size in chunks:
            got = [
                (dot_nn(picks[cc], tok[h, pair * 2 + cc, :, n : n + size]) * scales[cc]).reshape(32, 8, size)
                for cc in range(2)
            ]
            routed[h, :, to, n : n + size] = jnp.concatenate(got, axis=1).astype(BF)

    lane_expert = iota((64, 256), 1) // 32

    def wait_partner(k, dg):
        zz = source(k)
        for h in range(2):
            b = block(zz, turn(gather[h], dg), 1 - c)
            copy(meta.at[h, b], meta.at[h, b], mps.at[h, k, dg], mpr.at[h, k, dg], partner).wait_recv()
            copy(tok.at[h, b], tok.at[h, b], ps.at[h, k, dg], pr.at[h, k, dg], partner).wait_recv()

    def stage_c(k):
        zz = source(k)
        for dg in (0, 1, 3):
            wait_partner(k, dg)

        @pl.loop(0, 6)
        def _(i):
            h, n = i % 2, i // 2
            rows_of(h, zz, turn(jnp.where(h == 0, y, x), n + n // 2))

        wait_partner(k, 2)

        @pl.loop(0, 2)
        def _(h):
            rows_of(h, zz, turn(jnp.where(h == 0, y, x), 2))

        part = pl.ds(pl.multiple_of(zz * 64, 64), 64)
        for h in range(2):
            for r in (2, 1, 3, 0):
                to = turn(spread[h], r)
                rows = routed[h, pl.ds(to * 8, 8), part, :].reshape(512, width)
                every = dot_nt(rows, q_row[h, to])
                total = jnp.zeros((64, 256), F32)
                for j in range(8):
                    total = total + jnp.where(lane_expert == j, every[j * 64 : j * 64 + 64], 0.0)
                if k == 0 and r == 0:
                    m_in[h, 0, 0] = total.astype(BF)
                else:
                    m_out[h, k, r] = total.astype(BF)
                    go(
                        copy(
                            m_out.at[h, k, r], m_in.at[h, r, k], ms.at[h, k, r], mr.at[h, k, r],
                            dev(h, 0, r, zorder[k]),
                        )
                    )

    stage_a(0)
    for h in range(2):
        load_q[h].wait()
        b = spread[h]
        for r in (2, 1, 3):
            go(copy(q_row.at[h, b], q_row.at[h, b], qs.at[h, r], qr.at[h, r], dev(h, 0, r, 0)))
    stage_a(1)
    stage_b(0)
    stage_a(2)
    stage_h(0)
    stage_b(1)
    for h in range(2):
        for r in (1, 2, 3):
            b = turn(spread[h], 4 - r)
            copy(q_row.at[h, b], q_row.at[h, b], qs.at[h, r], qr.at[h, r], partner).wait_recv()
    stage_c(0)
    stage_a(3)
    stage_h(1)
    stage_b(2)
    stage_c(1)
    stage_h(2)
    stage_b(3)
    stage_c(2)
    stage_h(3)
    stage_c(3)

    while waits:
        waits.pop(0).wait_send()

    load_hid.wait()

    def selection(h):
        row, slot = iota((256, 192), 0), iota((256, 192), 1)
        back = turn(spread[h] + 4 - row // 64, 0)
        along = (row // 16) % 4
        yy, xx = (along, back) if h == 0 else (back, along)
        at = ((yy * 4 + xx) * 2 + (row // 8) % 2) * CAP + row % 8
        return jnp.where((at == slot) & (row % 8 < CAP), 1.0, 0.0).astype(BF)

    select = [selection(h) for h in range(2)]
    mixed = jnp.zeros((256, 192), F32)
    for h in range(2):
        parts = []
        for r in range(4):
            total = None
            for k in range(4):
                if k or r:
                    copy(
                        m_out.at[h, k, r], m_in.at[h, r, k], ms.at[h, k, r], mr.at[h, k, r], partner
                    ).wait_recv()
                got = m_in[h, r, k].astype(F32)
                total = got if total is None else total + got
            parts.append(total)
        raw = jnp.concatenate(parts, axis=0)
        top = raw.astype(BF)
        rest = (raw - top.astype(F32)).astype(BF)
        mixed = mixed + dot_tn(top, select[h]) + dot_tn(rest, select[h])
    m_t[...] = mixed.astype(BF)

    for r in (2, 1, 3, 0):
        to = turn(z, r)
        for i in range(2):
            j = to * 2 + i
            rows = m_t[pl.ds(pl.multiple_of(j * 32, 32), 32), :]
            got = dot_nn(rows, hid[j])
            if r:
                f_out[r, i * 32 : i * 32 + 32, :] = got.astype(BF)
            else:
                f_own[i * 32 : i * 32 + 32, :] = got
        if r:
            go(copy(f_out.at[r], f_in.at[r], fs.at[r], fr.at[r], dev(0, 0, 0, r)))
    total = f_own[...]
    for r in (1, 3, 2):
        copy(f_out.at[r], f_in.at[r], fs.at[r], fr.at[r], partner).wait_recv()
        total = total + f_in[r].astype(F32)
    f_all[z] = total.astype(BF)
    for r in (2, 1, 3):
        go(copy(f_all.at[z], f_all.at[z], gs.at[r], gr.at[r], dev(0, 0, 0, r)))

    mat = f_all[z]
    gram = dot_nt(mat, jnp.concatenate([mat, mat], axis=0))
    lane, row = iota((32, 128), 1), iota((32, 128), 0)
    eye = jnp.where(lane % 32 == row, 1.0, 0.0)
    work = jnp.where(lane >= 96, gram[32:64], jnp.where(lane >= 64, gram[0:32], eye))
    first = (lane // 32) % 2 == 0
    for k in range(32):
        one = work[:, 64 + k : 65 + k]
        two = work[:, 96 + k : 97 + k]
        factor = jnp.where(first, one / one[k : k + 1, :], two / two[k : k + 1, :])
        factor = jnp.where(row > k, factor, 0.0)
        work = work - factor * work[k : k + 1, :]
    one = jnp.sum(jnp.where(lane == 64 + row, work, 0.0), axis=1, keepdims=True)
    two = jnp.sum(jnp.where(lane == 96 + row, work, 0.0), axis=1, keepdims=True)
    low[z] = work * jnp.where(first, 1.0 / jnp.sqrt(one), 1.0 / jnp.sqrt(two))
    for r in (2, 1, 3):
        go(copy(low.at[z], low.at[z], ls.at[r], lr.at[r], dev(0, 0, 0, r)))

    for r in (0, 1, 3, 2):
        zz = turn(z, 4 - r)
        if r:
            copy(f_all.at[zz], f_all.at[zz], gs.at[r], gr.at[r], partner).wait_recv()
        for i in range(2):
            j = zz * 2 + i
            got = dot_nt(f_all[zz, i * 32 : i * 32 + 32, :], hid[j])
            hf[pl.ds(pl.multiple_of(j * 32, 32), 32), :] = got
    place64 = iota((32, 64), 1) < 32

    def lower(zz):
        both = low[zz][:, 0:64]
        return jnp.concatenate([jnp.where(place64, both, 0.0), jnp.where(place64, 0.0, both)], axis=0)

    for r in (0, 1, 3, 2):
        zz = turn(z, 4 - r)
        if r:
            copy(low.at[zz], low.at[zz], ls.at[r], lr.at[r], partner).wait_recv()
        at = pl.ds(pl.multiple_of(zz * 64, 64), 64)
        m_t[at, :] = dot_nn(lower(zz), hf[at, :], precision=HI).astype(BF)
    while waits:
        waits.pop(0).wait_send()
    for h in range(2):
        spreads = dot_nt(select[h], m_t[...]).astype(BF)
        for r in range(4):
            m_out[h, 0, r] = spreads[r * 64 : r * 64 + 64]
        p_in[h, 0, z] = spreads[0:64]
        for r in (2, 1, 3, 0):
            for q in (2, 1, 3, 0):
                if r or q:
                    go(
                        copy(
                            m_out.at[h, 0, r], p_in.at[h, r, z], js.at[h, r, q], jr.at[h, r, q],
                            dev(h, 0, 4 - r, q),
                        )
                    )
    for zz in range(4):
        mat = lower(zz)
        top = mat.astype(BF)
        rest = (mat - top.astype(F32)).astype(BF)
        basis_ref[zz * 64 : zz * 64 + 64, :] = (dot_nn(top, f_all[zz]) + dot_nn(rest, f_all[zz])).astype(BF)

    for r in (2, 1, 3, 0):
        for h in range(2):
            b = turn(spread[h], r)
            for q in range(4):
                if r or q:
                    zz = turn(z, 4 - q)
                    copy(m_out.at[h, 0, r], p_in.at[h, r, zz], js.at[h, r, q], jr.at[h, r, q], partner).wait_recv()
            terms = jnp.concatenate([p_in[h, r, zz] for zz in range(4)], axis=0)
            p_t[...] = terms.astype(F32).T.astype(BF)

            @pl.loop(0, 8)
            def _(j):
                at = pl.ds(pl.multiple_of(j * 32, 32), 32)
                got = dot_nn(p_t[at, :], routed[h, b * 8 + j])
                if r:
                    to = pl.ds(pl.multiple_of((j % 4) * 32, 32), 32)
                    tok[h, 2 * r + j // 4, to, :] = got.astype(BF)
                else:
                    update_ref[at, h * width : h * width + width] = got

            if r:
                go(
                    copy(
                        tok.at[h, pl.ds(2 * r, 2)], tok.at[h, pl.ds(8 + 2 * r, 2)], us.at[h, r], ur.at[h, r],
                        dev(h, 0, r, 0),
                    )
                )
    for r in (1, 3, 2):
        for h in range(2):
            copy(
                tok.at[h, pl.ds(2 * r, 2)], tok.at[h, pl.ds(8 + 2 * r, 2)], us.at[h, r], ur.at[h, r], partner
            ).wait_recv()

            @pl.loop(0, 8)
            def _(j):
                at = pl.ds(pl.multiple_of(j * 32, 32), 32)
                to = pl.ds(pl.multiple_of((j % 4) * 32, 32), 32)
                side = slice(h * width, h * width + width)
                update_ref[at, side] = update_ref[at, side] + tok[h, 8 + 2 * r + j // 4, to, :].astype(F32)

    for cp in waits:
        cp.wait_send()


def local(out_grads, expert_ids, gate_probs, hidden_acts, q_previous):
    experts, rank, model = q_previous.shape
    hidden_units = hidden_acts.shape[3]
    width = model // lax.axis_size("dp")
    half = width // 2
    any_spec, vmem = pl.BlockSpec(memory_space=pl.ANY), pl.BlockSpec(memory_space=pltpu.VMEM)
    dma = lambda *shape: pltpu.SemaphoreType.DMA(shape)
    basis, update = pl.pallas_call(
        kernel,
        out_shape=(
            jax.ShapeDtypeStruct((experts * rank, hidden_units), BF),
            jax.ShapeDtypeStruct((experts * rank, width), F32),
        ),
        in_specs=[vmem, vmem, any_spec, any_spec, any_spec],
        out_specs=(vmem, vmem),
        scratch_shapes=[
            pltpu.VMEM((2, 32, 128, half), BF),
            pltpu.VMEM((2, 32, 16, 128), F32),
            pltpu.VMEM((2, 4, 256, half), BF),
            pltpu.VMEM((2, 32, 256, half), BF),
            pltpu.VMEM((8, 192, hidden_units), BF),
            pltpu.VMEM((2, 4, 4, 64, 256), BF),
            pltpu.VMEM((2, 4, 4, 64, 256), BF),
            pltpu.VMEM((256, 192), BF),
            pltpu.VMEM((256, 192), F32),
            pltpu.VMEM((4, 64, hidden_units), BF),
            pltpu.VMEM((4, 64, hidden_units), BF),
            pltpu.VMEM((64, hidden_units), F32),
            pltpu.VMEM((4, 64, hidden_units), BF),
            pltpu.VMEM((4, 32, 128), F32),
            pltpu.VMEM((2, 4, 4, 64, 256), BF),
            pltpu.VMEM((256, 256), BF),
            dma(5),
            dma(2, 4), dma(2, 4), dma(2, 2, 4), dma(2, 2, 4), dma(2, 2, 4), dma(2, 2, 4), dma(2, 4, 4), dma(2, 4, 4),
            dma(2, 4), dma(2, 4), dma(2, 2, 4), dma(2, 2, 4), dma(2, 4), dma(2, 4), dma(2, 4, 4), dma(2, 4, 4),
            dma(2, 4), dma(2, 4), dma(2, 4, 4), dma(2, 4, 4), dma(4), dma(4), dma(4), dma(4), dma(4), dma(4),
            dma(2, 4, 4), dma(2, 4, 4), dma(2, 4), dma(2, 4),
        ],
        compiler_params=pltpu.CompilerParams(
            collective_id=0, has_side_effects=True, vmem_limit_bytes=67043328
        ),
    )(
        expert_ids[0].T,
        gate_probs[0].T,
        out_grads[0],
        hidden_acts[0],
        q_previous.reshape(experts * rank, model),
    )
    basis = basis.reshape(experts, rank, hidden_units).astype(F32) * math.sqrt(hidden_units)
    return (basis, update.reshape(experts, rank, width))


def solution(mesh):
    return jax.shard_map(
        local,
        mesh=mesh,
        in_specs=(
            P("dp", "expert", None),
            P("dp", "expert", None),
            P("dp", "expert", None),
            P("dp", "expert", None, None),
            P("expert", None, None),
        ),
        out_specs=(P("expert", None, None), P("expert", None, "dp")),
        check_vma=False,
    )
```

```python
import math

import jax
import jax.numpy as jnp
from jax import lax
from jax.experimental import pallas as pl
from jax.experimental.pallas import tpu as pltpu
from jax.sharding import PartitionSpec as P

MESH = pl.DeviceIdType.MESH
BF, F32 = jnp.bfloat16, jnp.float32
HI = lax.Precision.HIGHEST
SLOT = 8
CAP = 6


def dot_nt(left, right, **more):
    return lax.dot_general(left, right, (((1,), (1,)), ((), ())), preferred_element_type=F32, **more)


def dot_nn(left, right, **more):
    return lax.dot_general(left, right, (((1,), (0,)), ((), ())), preferred_element_type=F32, **more)


def dot_tn(left, right, **more):
    return lax.dot_general(left, right, (((0,), (0,)), ((), ())), preferred_element_type=F32, **more)


def iota(shape, dim):
    return lax.broadcasted_iota(jnp.int32, shape, dim)


def kernel(
    ids_ref, gates_ref, grads_ref, hidden_ref, prev_ref, basis_ref, update_ref,
    tok, meta, q_row, routed, hid, m_out, m_in, m_t, hf, f_out, f_in, f_own, f_all, low, p_in, p_t,
    load_sem, zs, zr, as_, ar, hs, hr, ps, pr,
    mzs, mzr, mas, mar, mhs, mhr, mps, mpr,
    qs, qr, ms, mr, fs, fr, gs, gr, ls, lr, js, jr, us, ur,
):
    width = tok.shape[3]
    e, z = lax.axis_index("expert"), lax.axis_index("dp")
    y, x, c = e // 8, (e // 2) % 4, e % 2
    gather, spread = (y, x), (x, y)

    def turn(v, by):
        return lax.rem(v + by, 4)

    def dev(h, along_gather, along_spread, to_z, core=0):
        g, s = turn(gather[h], along_gather), turn(spread[h], along_spread)
        yy, xx = (g, s) if h == 0 else (s, g)
        cc = 1 - c if core else c
        return {"expert": (yy * 4 + xx) * 2 + cc, "dp": turn(z, to_z)}

    def copy(src, dst, send, recv, device):
        return pltpu.make_async_remote_copy(src, dst, send, recv, device_id=device, device_id_type=MESH)

    def block(zz, gg, cc):
        return (zz * 4 + gg) * 2 + cc

    def cols(zz, h):
        return pl.ds(pl.multiple_of(zz * (2 * width) + h * width, 128), width)

    own = [block(z, gather[h], c) for h in range(2)]
    load_tok = [
        pltpu.make_async_copy(grads_ref.at[:, cols(z, h)], tok.at[h, own[h]], load_sem.at[h])
        for h in range(2)
    ]
    load_q = [
        pltpu.make_async_copy(prev_ref.at[:, cols(z, h)], q_row.at[h, spread[h]], load_sem.at[2 + h])
        for h in range(2)
    ]
    load_hid = pltpu.make_async_copy(hidden_ref, hid, load_sem.at[4])
    for cp in load_tok + load_q + [load_hid]:
        cp.start()

    barrier = pltpu.get_barrier_semaphore()
    peers = [dev(0, 0, 0, 0, core=1)] + [dev(0, 0, 0, r) for r in (1, 2, 3)]
    for h in range(2):
        for b in (1, 2, 3):
            for r in range(4):
                peers.append(dev(h, 0, b, r))
    for peer in peers:
        pl.semaphore_signal(barrier, inc=1, device_id=peer, device_id_type=MESH)

    ids = ids_ref[...]
    expert_row = iota((256, 128), 0)
    named = jnp.zeros((256, 128), F32)
    for k in range(8):
        named = named + jnp.where(ids[k : k + 1, :] == expert_row, 1.0, 0.0)
    before = jnp.where(iota((128, 128), 0) < iota((128, 128), 1), 1.0, 0.0).astype(BF)
    earlier = dot_nn(named.astype(BF), before)
    place = jnp.concatenate(
        [
            jnp.sum(jnp.where(ids[k : k + 1, :] == expert_row, earlier, 0.0), axis=0, keepdims=True)
            for k in range(8)
        ],
        axis=0,
    )
    holder, inner = ids // 8, ids % 8
    at_y, at_x, at_c = holder // 8, (holder // 2) % 4, holder % 2
    for h, (g, s) in enumerate(((at_y, at_x), (at_x, at_y))):
        base = (g * 2 + at_c) * 256 + (s * 8 + inner) * SLOT
        meta[h, own[h], 0:8, :] = base.astype(F32) + place
        meta[h, own[h], 8:16, :] = gates_ref[...]

    pl.semaphore_wait(barrier, len(peers))

    waits = []

    def go(cp):
        cp.start()
        waits.append(cp)

    zorder = [1, 3, 2, 0]
    for h in range(2):
        load_q[h].wait()
        b = spread[h]
        for way in range(2):
            go(copy(q_row.at[h, b], q_row.at[h, b], qs.at[h, way], qr.at[h, way], dev(h, 0, 1 + 2 * way, 0)))
    for r in (1, 3, 2):
        for h in range(2):
            b = own[h]
            to = turn(z, r)
            go(copy(meta.at[h, b], meta.at[h, b], mzs.at[h, r], mzr.at[h, r], dev(0, 0, 0, r)))
            go(copy(grads_ref.at[:, cols(to, h)], tok.at[h, b], zs.at[h, r], zr.at[h, r], dev(0, 0, 0, r)))

    partner = dev(0, 0, 0, 0, core=1)

    def to_partner(h, k, zz, dg):
        b = block(zz, turn(gather[h], dg), c)
        go(copy(meta.at[h, b], meta.at[h, b], mps.at[h, k, dg], mpr.at[h, k, dg], partner))
        go(copy(tok.at[h, b], tok.at[h, b], ps.at[h, k, dg], pr.at[h, k, dg], partner))

    def source(k):
        return turn(z, zorder[k])

    def stage_a(k):
        zz = source(k)
        for h in range(2):
            b = block(zz, gather[h], c)
            if zorder[k]:
                r = (4 - zorder[k]) % 4
                copy(meta.at[h, b], meta.at[h, b], mzs.at[h, r], mzr.at[h, r], partner).wait_recv()
                copy(tok.at[h, b], tok.at[h, b], zs.at[h, r], zr.at[h, r], partner).wait_recv()
            else:
                load_tok[h].wait()
            for way, step in ((0, 1), (1, 3)):
                device = dev(h, step, 0, 0)
                go(copy(meta.at[h, b], meta.at[h, b], mas.at[h, way, k], mar.at[h, way, k], device))
                go(copy(tok.at[h, b], tok.at[h, b], as_.at[h, way, k], ar.at[h, way, k], device))
            to_partner(h, k, zz, 0)

    def stage_b(k):
        zz = source(k)
        for h in range(2):
            for way, step, dg in ((0, 1, 3), (1, 3, 1)):
                device = dev(h, step, 0, 0)
                b = block(zz, turn(gather[h], dg), c)
                copy(meta.at[h, b], meta.at[h, b], mas.at[h, way, k], mar.at[h, way, k], device).wait_recv()
                copy(tok.at[h, b], tok.at[h, b], as_.at[h, way, k], ar.at[h, way, k], device).wait_recv()
                half = pl.ds(way * 64, 64)
                if way == 0:
                    go(copy(meta.at[h, b], meta.at[h, b], mhs.at[h, k], mhr.at[h, k], device))
                go(copy(tok.at[h, b, half], tok.at[h, b, half], hs.at[h, way, k], hr.at[h, way, k], device))
                to_partner(h, k, zz, dg)

    def stage_h(k):
        zz = source(k)
        for h in range(2):
            b = block(zz, turn(gather[h], 2), c)
            copy(meta.at[h, b], meta.at[h, b], mhs.at[h, k], mhr.at[h, k], partner).wait_recv()
            for way in range(2):
                half = pl.ds(way * 64, 64)
                copy(
                    tok.at[h, b, half], tok.at[h, b, half], hs.at[h, way, k], hr.at[h, way, k], partner
                ).wait_recv()
            to_partner(h, k, zz, 2)

    mine = [((gather[h] * 2 + c) * 256).astype(F32) for h in range(2)]
    row_of = iota((256, 128), 0).astype(F32)
    chunks = [(n, min(256, width - n)) for n in range(0, width, 256)]

    def rows_of(h, zz, gg):
        pair = zz * 4 + gg
        less = jnp.where(h == 0, mine[0], mine[1])
        picks, scales = [], []
        for cc in range(2):
            info = meta[h, pair * 2 + cc]
            want = info[0:8] - less
            gate = jnp.zeros((256, 128), F32)
            for k in range(8):
                gate = jnp.where(row_of == want[k : k + 1], info[8 + k : 9 + k], gate)
            picks.append(jnp.where(gate > 0.0, 1.0, 0.0).astype(BF))
            scales.append(jnp.sum(gate, axis=1, keepdims=True))
        to = pl.ds(pl.multiple_of(pair * 16, 16), 16)
        for n, size in chunks:
            got = [
                (dot_nn(picks[cc], tok[h, pair * 2 + cc, :, n : n + size]) * scales[cc]).reshape(32, 8, size)
                for cc in range(2)
            ]
            routed[h, :, to, n : n + size] = jnp.concatenate(got, axis=1).astype(BF)

    lane_expert = iota((64, 256), 1) // 32

    def wait_partner(k, dg):
        zz = source(k)
        for h in range(2):
            b = block(zz, turn(gather[h], dg), 1 - c)
            copy(meta.at[h, b], meta.at[h, b], mps.at[h, k, dg], mpr.at[h, k, dg], partner).wait_recv()
            copy(tok.at[h, b], tok.at[h, b], ps.at[h, k, dg], pr.at[h, k, dg], partner).wait_recv()

    def stage_rows(k):
        zz = source(k)
        for dg in (0, 1, 3):
            wait_partner(k, dg)

        @pl.loop(0, 6)
        def _(i):
            h, n = i % 2, i // 2
            rows_of(h, zz, turn(jnp.where(h == 0, y, x), n + n // 2))

        wait_partner(k, 2)

        @pl.loop(0, 2)
        def _(h):
            rows_of(h, zz, turn(jnp.where(h == 0, y, x), 2))

    def stage_mix(k):
        zz = source(k)
        part = pl.ds(pl.multiple_of(zz * 64, 64), 64)
        for h in range(2):
            for r in (2, 1, 3, 0):
                to = turn(spread[h], r)
                rows = routed[h, pl.ds(to * 8, 8), part, :].reshape(512, width)
                every = dot_nt(rows, q_row[h, to])
                total = jnp.zeros((64, 256), F32)
                for j in range(8):
                    total = total + jnp.where(lane_expert == j, every[j * 64 : j * 64 + 64], 0.0)
                if zorder[k] == 0 and r == 0:
                    m_in[h, 0, k] = total.astype(BF)
                else:
                    m_out[h, k, r] = total.astype(BF)
                    go(
                        copy(
                            m_out.at[h, k, r], m_in.at[h, r, k], ms.at[h, k, r], mr.at[h, k, r],
                            dev(h, 0, r, zorder[k]),
                        )
                    )

    for h in range(2):
        for way, back in ((0, 3), (1, 1)):
            b = turn(spread[h], back)
            copy(q_row.at[h, b], q_row.at[h, b], qs.at[h, way], qr.at[h, way], partner).wait_recv()
            part = pl.ds(way * 128, 128)
            go(
                copy(
                    q_row.at[h, b, part], q_row.at[h, b, part], qs.at[h, 2 + way], qr.at[h, 2 + way],
                    dev(h, 0, 1 + 2 * way, 0),
                )
            )
    stage_a(0)
    stage_a(1)
    stage_b(0)
    stage_a(2)
    stage_h(0)
    stage_b(1)
    stage_a(3)
    stage_rows(0)
    stage_h(1)
    stage_b(2)
    for h in range(2):
        b = turn(spread[h], 2)
        for way in range(2):
            part = pl.ds(way * 128, 128)
            copy(
                q_row.at[h, b, part], q_row.at[h, b, part], qs.at[h, 2 + way], qr.at[h, 2 + way], partner
            ).wait_recv()
    stage_mix(0)
    stage_rows(1)
    stage_h(2)
    stage_b(3)
    stage_mix(1)
    stage_rows(2)
    stage_h(3)
    stage_mix(2)
    stage_rows(3)
    stage_mix(3)

    while waits:
        waits.pop(0).wait_send()

    load_hid.wait()

    def selection(h):
        row, slot = iota((256, 192), 0), iota((256, 192), 1)
        back = turn(spread[h] + 4 - row // 64, 0)
        along = (row // 16) % 4
        yy, xx = (along, back) if h == 0 else (back, along)
        at = ((yy * 4 + xx) * 2 + (row // 8) % 2) * CAP + row % 8
        return jnp.where((at == slot) & (row % 8 < CAP), 1.0, 0.0).astype(BF)

    select = [selection(h) for h in range(2)]
    mixed = jnp.zeros((256, 192), F32)
    for h in range(2):
        parts = []
        for r in range(4):
            total = None
            for k in range(4):
                if zorder[k] or r:
                    copy(
                        m_out.at[h, k, r], m_in.at[h, r, k], ms.at[h, k, r], mr.at[h, k, r], partner
                    ).wait_recv()
                got = m_in[h, r, k].astype(F32)
                total = got if total is None else total + got
            parts.append(total)
        raw = jnp.concatenate(parts, axis=0)
        top = raw.astype(BF)
        rest = (raw - top.astype(F32)).astype(BF)
        mixed = mixed + dot_tn(top, select[h]) + dot_tn(rest, select[h])
    m_t[...] = mixed.astype(BF)

    for r in (2, 1, 3, 0):
        to = turn(z, r)
        for i in range(2):
            j = to * 2 + i
            rows = m_t[pl.ds(pl.multiple_of(j * 32, 32), 32), :]
            got = dot_nn(rows, hid[j])
            if r:
                f_out[r, i * 32 : i * 32 + 32, :] = got.astype(BF)
            else:
                f_own[i * 32 : i * 32 + 32, :] = got
        if r:
            go(copy(f_out.at[r], f_in.at[r], fs.at[r], fr.at[r], dev(0, 0, 0, r)))
    total = f_own[...]
    for r in (1, 3, 2):
        copy(f_out.at[r], f_in.at[r], fs.at[r], fr.at[r], partner).wait_recv()
        total = total + f_in[r].astype(F32)
    f_all[z] = total.astype(BF)
    for r in (2, 1, 3):
        go(copy(f_all.at[z], f_all.at[z], gs.at[r], gr.at[r], dev(0, 0, 0, r)))

    mat = f_all[z]
    gram = dot_nt(mat, jnp.concatenate([mat, mat], axis=0))
    lane, row = iota((32, 128), 1), iota((32, 128), 0)
    eye = jnp.where(lane % 32 == row, 1.0, 0.0)
    work = jnp.where(lane >= 96, gram[32:64], jnp.where(lane >= 64, gram[0:32], eye))
    first = (lane // 32) % 2 == 0
    for k in range(32):
        one = work[:, 64 + k : 65 + k]
        two = work[:, 96 + k : 97 + k]
        factor = jnp.where(first, one / one[k : k + 1, :], two / two[k : k + 1, :])
        factor = jnp.where(row > k, factor, 0.0)
        work = work - factor * work[k : k + 1, :]
    one = jnp.sum(jnp.where(lane == 64 + row, work, 0.0), axis=1, keepdims=True)
    two = jnp.sum(jnp.where(lane == 96 + row, work, 0.0), axis=1, keepdims=True)
    low[z] = work * jnp.where(first, 1.0 / jnp.sqrt(one), 1.0 / jnp.sqrt(two))
    for r in (2, 1, 3):
        go(copy(low.at[z], low.at[z], ls.at[r], lr.at[r], dev(0, 0, 0, r)))

    for r in (0, 1, 3, 2):
        zz = turn(z, 4 - r)
        if r:
            copy(f_all.at[zz], f_all.at[zz], gs.at[r], gr.at[r], partner).wait_recv()
        for i in range(2):
            j = zz * 2 + i
            got = dot_nt(f_all[zz, i * 32 : i * 32 + 32, :], hid[j])
            hf[pl.ds(pl.multiple_of(j * 32, 32), 32), :] = got
    place64 = iota((32, 64), 1) < 32

    def lower(zz):
        both = low[zz][:, 0:64]
        return jnp.concatenate([jnp.where(place64, both, 0.0), jnp.where(place64, 0.0, both)], axis=0)

    for r in (0, 1, 3, 2):
        zz = turn(z, 4 - r)
        if r:
            copy(low.at[zz], low.at[zz], ls.at[r], lr.at[r], partner).wait_recv()
        at = pl.ds(pl.multiple_of(zz * 64, 64), 64)
        m_t[at, :] = dot_nn(lower(zz), hf[at, :], precision=HI).astype(BF)
    while waits:
        waits.pop(0).wait_send()
    while waits:
        waits.pop(0).wait_send()
    for h in range(2):
        spreads = dot_nt(select[h], m_t[...]).astype(BF)
        for r in range(4):
            m_out[h, 0, r] = spreads[r * 64 : r * 64 + 64]
        p_in[h, 0, z] = spreads[0:64]
        for r in (2, 1, 3, 0):
            for q in (2, 1, 3, 0):
                if r or q:
                    go(
                        copy(
                            m_out.at[h, 0, r], p_in.at[h, r, z], js.at[h, r, q], jr.at[h, r, q],
                            dev(h, 0, 4 - r, q),
                        )
                    )
    for zz in range(4):
        mat = lower(zz)
        top = mat.astype(BF)
        rest = (mat - top.astype(F32)).astype(BF)
        basis_ref[zz * 64 : zz * 64 + 64, :] = (dot_nn(top, f_all[zz]) + dot_nn(rest, f_all[zz])).astype(BF)

    for r in (2, 1, 3, 0):
        for h in range(2):
            b = turn(spread[h], r)
            for q in range(4):
                if r or q:
                    zz = turn(z, 4 - q)
                    copy(m_out.at[h, 0, r], p_in.at[h, r, zz], js.at[h, r, q], jr.at[h, r, q], partner).wait_recv()
            terms = jnp.concatenate([p_in[h, r, zz] for zz in range(4)], axis=0)
            p_t[...] = terms.astype(F32).T.astype(BF)

            @pl.loop(0, 8)
            def _(j):
                at = pl.ds(pl.multiple_of(j * 32, 32), 32)
                got = dot_nn(p_t[at, :], routed[h, b * 8 + j])
                if r:
                    to = pl.ds(pl.multiple_of((j % 4) * 32, 32), 32)
                    tok[h, 2 * r + j // 4, to, :] = got.astype(BF)
                else:
                    update_ref[at, h * width : h * width + width] = got

            if r:
                go(
                    copy(
                        tok.at[h, pl.ds(2 * r, 2)], tok.at[h, pl.ds(8 + 2 * r, 2)], us.at[h, r], ur.at[h, r],
                        dev(h, 0, r, 0),
                    )
                )
    for r in (1, 3, 2):
        for h in range(2):
            copy(
                tok.at[h, pl.ds(2 * r, 2)], tok.at[h, pl.ds(8 + 2 * r, 2)], us.at[h, r], ur.at[h, r], partner
            ).wait_recv()

            @pl.loop(0, 8)
            def _(j):
                at = pl.ds(pl.multiple_of(j * 32, 32), 32)
                to = pl.ds(pl.multiple_of((j % 4) * 32, 32), 32)
                side = slice(h * width, h * width + width)
                update_ref[at, side] = update_ref[at, side] + tok[h, 8 + 2 * r + j // 4, to, :].astype(F32)

    for cp in waits:
        cp.wait_send()


def local(out_grads, expert_ids, gate_probs, hidden_acts, q_previous):
    experts, rank, model = q_previous.shape
    hidden_units = hidden_acts.shape[3]
    width = model // lax.axis_size("dp")
    half = width // 2
    any_spec, vmem = pl.BlockSpec(memory_space=pl.ANY), pl.BlockSpec(memory_space=pltpu.VMEM)
    dma = lambda *shape: pltpu.SemaphoreType.DMA(shape)
    basis, update = pl.pallas_call(
        kernel,
        out_shape=(
            jax.ShapeDtypeStruct((experts * rank, hidden_units), BF),
            jax.ShapeDtypeStruct((experts * rank, width), F32),
        ),
        in_specs=[vmem, vmem, any_spec, any_spec, any_spec],
        out_specs=(vmem, vmem),
        scratch_shapes=[
            pltpu.VMEM((2, 32, 128, half), BF),
            pltpu.VMEM((2, 32, 16, 128), F32),
            pltpu.VMEM((2, 4, 256, half), BF),
            pltpu.VMEM((2, 32, 256, half), BF),
            pltpu.VMEM((8, 192, hidden_units), BF),
            pltpu.VMEM((2, 4, 4, 64, 256), BF),
            pltpu.VMEM((2, 4, 4, 64, 256), BF),
            pltpu.VMEM((256, 192), BF),
            pltpu.VMEM((256, 192), F32),
            pltpu.VMEM((4, 64, hidden_units), BF),
            pltpu.VMEM((4, 64, hidden_units), BF),
            pltpu.VMEM((64, hidden_units), F32),
            pltpu.VMEM((4, 64, hidden_units), BF),
            pltpu.VMEM((4, 32, 128), F32),
            pltpu.VMEM((2, 4, 4, 64, 256), BF),
            pltpu.VMEM((256, 256), BF),
            dma(5),
            dma(2, 4), dma(2, 4), dma(2, 2, 4), dma(2, 2, 4), dma(2, 2, 4), dma(2, 2, 4), dma(2, 4, 4), dma(2, 4, 4),
            dma(2, 4), dma(2, 4), dma(2, 2, 4), dma(2, 2, 4), dma(2, 4), dma(2, 4), dma(2, 4, 4), dma(2, 4, 4),
            dma(2, 4), dma(2, 4), dma(2, 4, 4), dma(2, 4, 4), dma(4), dma(4), dma(4), dma(4), dma(4), dma(4),
            dma(2, 4, 4), dma(2, 4, 4), dma(2, 4), dma(2, 4),
        ],
        compiler_params=pltpu.CompilerParams(
            collective_id=0, has_side_effects=True, vmem_limit_bytes=67043328
        ),
    )(
        expert_ids[0].T,
        gate_probs[0].T,
        out_grads[0],
        hidden_acts[0],
        q_previous.reshape(experts * rank, model),
    )
    basis = basis.reshape(experts, rank, hidden_units).astype(F32) * math.sqrt(hidden_units)
    return (basis, update.reshape(experts, rank, width))


def solution(mesh):
    return jax.shard_map(
        local,
        mesh=mesh,
        in_specs=(
            P("dp", "expert", None),
            P("dp", "expert", None),
            P("dp", "expert", None),
            P("dp", "expert", None, None),
            P("expert", None, None),
        ),
        out_specs=(P("expert", None, None), P("expert", None, "dp")),
        check_vma=False,
    )
```

```python
import math

import jax
import jax.numpy as jnp
from jax import lax
from jax.experimental import pallas as pl
from jax.experimental.pallas import tpu as pltpu
from jax.sharding import PartitionSpec as P

MESH = pl.DeviceIdType.MESH
BF, F32 = jnp.bfloat16, jnp.float32
HI = lax.Precision.HIGHEST
SLOT = 8
CAP = 6


def dot_nt(left, right, **more):
    return lax.dot_general(left, right, (((1,), (1,)), ((), ())), preferred_element_type=F32, **more)


def dot_nn(left, right, **more):
    return lax.dot_general(left, right, (((1,), (0,)), ((), ())), preferred_element_type=F32, **more)


def dot_tn(left, right, **more):
    return lax.dot_general(left, right, (((0,), (0,)), ((), ())), preferred_element_type=F32, **more)


def iota(shape, dim):
    return lax.broadcasted_iota(jnp.int32, shape, dim)


def kernel(
    ids_ref, gates_ref, grads_ref, hidden_ref, prev_ref, basis_ref, update_ref,
    tok, meta, q_row, routed, hid, m_out, m_in, m_t, hf, f_out, f_in, f_own, f_all, low, p_in, p_t,
    load_sem, zs, zr, as_, ar, hs, hr, ps, pr,
    mzs, mzr, mas, mar, mhs, mhr, mps, mpr,
    qs, qr, ms, mr, fs, fr, gs, gr, ls, lr, js, jr, us, ur,
):
    width = tok.shape[3]
    e, z = lax.axis_index("expert"), lax.axis_index("dp")
    y, x, c = e // 8, (e // 2) % 4, e % 2
    gather, spread = (y, x), (x, y)

    def turn(v, by):
        return lax.rem(v + by, 4)

    def dev(h, along_gather, along_spread, to_z, core=0):
        g, s = turn(gather[h], along_gather), turn(spread[h], along_spread)
        yy, xx = (g, s) if h == 0 else (s, g)
        cc = 1 - c if core else c
        return {"expert": (yy * 4 + xx) * 2 + cc, "dp": turn(z, to_z)}

    def copy(src, dst, send, recv, device):
        return pltpu.make_async_remote_copy(src, dst, send, recv, device_id=device, device_id_type=MESH)

    def block(zz, gg, cc):
        return (zz * 4 + gg) * 2 + cc

    def cols(zz, h):
        return pl.ds(pl.multiple_of(zz * (2 * width) + h * width, 128), width)

    own = [block(z, gather[h], c) for h in range(2)]
    load_tok = [
        pltpu.make_async_copy(grads_ref.at[:, cols(z, h)], tok.at[h, own[h]], load_sem.at[h])
        for h in range(2)
    ]
    load_q = [
        pltpu.make_async_copy(prev_ref.at[:, cols(z, h)], q_row.at[h, spread[h]], load_sem.at[2 + h])
        for h in range(2)
    ]
    load_hid = pltpu.make_async_copy(hidden_ref, hid, load_sem.at[4])
    for cp in load_tok + load_q + [load_hid]:
        cp.start()

    barrier = pltpu.get_barrier_semaphore()
    peers = [dev(0, 0, 0, 0, core=1)] + [dev(0, 0, 0, r) for r in (1, 2, 3)]
    for h in range(2):
        for b in (1, 2, 3):
            for r in range(4):
                peers.append(dev(h, 0, b, r))
    for peer in peers:
        pl.semaphore_signal(barrier, inc=1, device_id=peer, device_id_type=MESH)

    ids = ids_ref[...]
    expert_row = iota((256, 128), 0)
    named = jnp.zeros((256, 128), F32)
    for k in range(8):
        named = named + jnp.where(ids[k : k + 1, :] == expert_row, 1.0, 0.0)
    before = jnp.where(iota((128, 128), 0) < iota((128, 128), 1), 1.0, 0.0).astype(BF)
    earlier = dot_nn(named.astype(BF), before)
    place = jnp.concatenate(
        [
            jnp.sum(jnp.where(ids[k : k + 1, :] == expert_row, earlier, 0.0), axis=0, keepdims=True)
            for k in range(8)
        ],
        axis=0,
    )
    holder, inner = ids // 8, ids % 8
    at_y, at_x, at_c = holder // 8, (holder // 2) % 4, holder % 2
    for h, (g, s) in enumerate(((at_y, at_x), (at_x, at_y))):
        base = (g * 2 + at_c) * 256 + (s * 8 + inner) * SLOT
        meta[h, own[h], 0:8, :] = base.astype(F32) + place
        meta[h, own[h], 8:16, :] = gates_ref[...]

    pl.semaphore_wait(barrier, len(peers))

    waits = []

    def go(cp):
        cp.start()
        waits.append(cp)

    zorder = [1, 3, 2, 0]
    for h in range(2):
        load_q[h].wait()
        b = spread[h]
        for way in range(2):
            go(copy(q_row.at[h, b], q_row.at[h, b], qs.at[h, way], qr.at[h, way], dev(h, 0, 1 + 2 * way, 0)))
    for r in (1, 3, 2):
        for h in range(2):
            b = own[h]
            to = turn(z, r)
            go(copy(meta.at[h, b], meta.at[h, b], mzs.at[h, r], mzr.at[h, r], dev(0, 0, 0, r)))
            go(copy(grads_ref.at[:, cols(to, h)], tok.at[h, b], zs.at[h, r], zr.at[h, r], dev(0, 0, 0, r)))

    partner = dev(0, 0, 0, 0, core=1)

    def to_partner(h, k, zz, dg):
        b = block(zz, turn(gather[h], dg), c)
        go(copy(meta.at[h, b], meta.at[h, b], mps.at[h, k, dg], mpr.at[h, k, dg], partner))
        go(copy(tok.at[h, b], tok.at[h, b], ps.at[h, k, dg], pr.at[h, k, dg], partner))

    def source(k):
        return turn(z, zorder[k])

    def stage_a(k):
        zz = source(k)
        for h in range(2):
            b = block(zz, gather[h], c)
            if zorder[k]:
                r = (4 - zorder[k]) % 4
                copy(meta.at[h, b], meta.at[h, b], mzs.at[h, r], mzr.at[h, r], partner).wait_recv()
                copy(tok.at[h, b], tok.at[h, b], zs.at[h, r], zr.at[h, r], partner).wait_recv()
            else:
                load_tok[h].wait()
            for way, step in ((0, 1), (1, 3)):
                device = dev(h, step, 0, 0)
                go(copy(meta.at[h, b], meta.at[h, b], mas.at[h, way, k], mar.at[h, way, k], device))
                go(copy(tok.at[h, b], tok.at[h, b], as_.at[h, way, k], ar.at[h, way, k], device))
            to_partner(h, k, zz, 0)

    def stage_b(k):
        zz = source(k)
        for h in range(2):
            for way, step, dg in ((0, 1, 3), (1, 3, 1)):
                device = dev(h, step, 0, 0)
                b = block(zz, turn(gather[h], dg), c)
                copy(meta.at[h, b], meta.at[h, b], mas.at[h, way, k], mar.at[h, way, k], device).wait_recv()
                copy(tok.at[h, b], tok.at[h, b], as_.at[h, way, k], ar.at[h, way, k], device).wait_recv()
                half = pl.ds(way * 64, 64)
                if way == 0:
                    go(copy(meta.at[h, b], meta.at[h, b], mhs.at[h, k], mhr.at[h, k], device))
                go(copy(tok.at[h, b, half], tok.at[h, b, half], hs.at[h, way, k], hr.at[h, way, k], device))
                to_partner(h, k, zz, dg)

    def stage_h(k):
        zz = source(k)
        for h in range(2):
            b = block(zz, turn(gather[h], 2), c)
            copy(meta.at[h, b], meta.at[h, b], mhs.at[h, k], mhr.at[h, k], partner).wait_recv()
            for way in range(2):
                half = pl.ds(way * 64, 64)
                copy(
                    tok.at[h, b, half], tok.at[h, b, half], hs.at[h, way, k], hr.at[h, way, k], partner
                ).wait_recv()
            to_partner(h, k, zz, 2)

    mine = [((gather[h] * 2 + c) * 256).astype(F32) for h in range(2)]
    row_of = iota((256, 128), 0).astype(F32)
    chunks = [(n, min(256, width - n)) for n in range(0, width, 256)]

    def rows_of(h, zz, gg):
        pair = zz * 4 + gg
        less = jnp.where(h == 0, mine[0], mine[1])
        picks, scales = [], []
        for cc in range(2):
            info = meta[h, pair * 2 + cc]
            want = info[0:8] - less
            gate = jnp.zeros((256, 128), F32)
            for k in range(8):
                gate = jnp.where(row_of == want[k : k + 1], info[8 + k : 9 + k], gate)
            picks.append(jnp.where(gate > 0.0, 1.0, 0.0).astype(BF))
            scales.append(jnp.sum(gate, axis=1, keepdims=True))
        to = pl.ds(pl.multiple_of(pair * 16, 16), 16)
        for n, size in chunks:
            got = [
                (dot_nn(picks[cc], tok[h, pair * 2 + cc, :, n : n + size]) * scales[cc]).reshape(32, 8, size)
                for cc in range(2)
            ]
            routed[h, :, to, n : n + size] = jnp.concatenate(got, axis=1).astype(BF)

    lane_expert = iota((64, 256), 1) // 32

    def wait_partner(k, dg):
        zz = source(k)
        for h in range(2):
            b = block(zz, turn(gather[h], dg), 1 - c)
            copy(meta.at[h, b], meta.at[h, b], mps.at[h, k, dg], mpr.at[h, k, dg], partner).wait_recv()
            copy(tok.at[h, b], tok.at[h, b], ps.at[h, k, dg], pr.at[h, k, dg], partner).wait_recv()

    def stage_rows(k):
        zz = source(k)
        for dg in (0, 1, 3):
            wait_partner(k, dg)

        @pl.loop(0, 6)
        def _(i):
            h, n = i % 2, i // 2
            rows_of(h, zz, turn(jnp.where(h == 0, y, x), n + n // 2))

        wait_partner(k, 2)

        @pl.loop(0, 2)
        def _(h):
            rows_of(h, zz, turn(jnp.where(h == 0, y, x), 2))

    def stage_mix(k):
        zz = source(k)
        part = pl.ds(pl.multiple_of(zz * 64, 64), 64)
        for h in range(2):
            for r in (2, 1, 3, 0):
                to = turn(spread[h], r)
                rows = routed[h, pl.ds(to * 8, 8), part, :].reshape(512, width)
                every = dot_nt(rows, q_row[h, to])
                total = jnp.zeros((64, 256), F32)
                for j in range(8):
                    total = total + jnp.where(lane_expert == j, every[j * 64 : j * 64 + 64], 0.0)
                if zorder[k] == 0 and r == 0:
                    m_in[h, 0, k] = total.astype(BF)
                else:
                    m_out[h, k, r] = total.astype(BF)
                    go(
                        copy(
                            m_out.at[h, k, r], m_in.at[h, r, k], ms.at[h, k, r], mr.at[h, k, r],
                            dev(h, 0, r, zorder[k]),
                        )
                    )

    for h in range(2):
        for way, back in ((0, 3), (1, 1)):
            b = turn(spread[h], back)
            copy(q_row.at[h, b], q_row.at[h, b], qs.at[h, way], qr.at[h, way], partner).wait_recv()
            part = pl.ds(way * 128, 128)
            go(
                copy(
                    q_row.at[h, b, part], q_row.at[h, b, part], qs.at[h, 2 + way], qr.at[h, 2 + way],
                    dev(h, 0, 1 + 2 * way, 0),
                )
            )
    stage_a(0)
    stage_a(1)
    stage_b(0)
    stage_a(2)
    stage_h(0)
    stage_b(1)
    stage_a(3)
    stage_rows(0)
    stage_h(1)
    stage_b(2)
    for h in range(2):
        b = turn(spread[h], 2)
        for way in range(2):
            part = pl.ds(way * 128, 128)
            copy(
                q_row.at[h, b, part], q_row.at[h, b, part], qs.at[h, 2 + way], qr.at[h, 2 + way], partner
            ).wait_recv()
    stage_mix(0)
    stage_rows(1)
    stage_h(2)
    stage_b(3)
    stage_mix(1)
    stage_rows(2)
    stage_h(3)
    stage_mix(2)
    stage_rows(3)
    stage_mix(3)

    while waits:
        waits.pop(0).wait_send()

    load_hid.wait()

    def selection(h):
        row, slot = iota((256, 192), 0), iota((256, 192), 1)
        back = turn(spread[h] + 4 - row // 64, 0)
        along = (row // 16) % 4
        yy, xx = (along, back) if h == 0 else (back, along)
        at = ((yy * 4 + xx) * 2 + (row // 8) % 2) * CAP + row % 8
        return jnp.where((at == slot) & (row % 8 < CAP), 1.0, 0.0).astype(BF)

    select = [selection(h) for h in range(2)]
    mixed = jnp.zeros((256, 192), F32)
    for h in range(2):
        parts = []
        for r in range(4):
            total = None
            for k in range(4):
                if zorder[k] or r:
                    copy(
                        m_out.at[h, k, r], m_in.at[h, r, k], ms.at[h, k, r], mr.at[h, k, r], partner
                    ).wait_recv()
                got = m_in[h, r, k].astype(F32)
                total = got if total is None else total + got
            parts.append(total)
        raw = jnp.concatenate(parts, axis=0)
        top = raw.astype(BF)
        rest = (raw - top.astype(F32)).astype(BF)
        mixed = mixed + dot_tn(top, select[h]) + dot_tn(rest, select[h])
    m_t[...] = mixed.astype(BF)

    units = hid.shape[2] // 2
    for u in range(2):
        for r in (2, 1, 3, 0):
            to = turn(z, r)
            for i in range(2):
                j = to * 2 + i
                rows = m_t[pl.ds(pl.multiple_of(j * 32, 32), 32), :]
                got = dot_nn(rows, hid[j, :, u * units : u * units + units])
                if r:
                    f_out[r, u, i * 32 : i * 32 + 32, :] = got.astype(BF)
                else:
                    f_own[u, i * 32 : i * 32 + 32, :] = got
            if r:
                go(copy(f_out.at[r, u], f_in.at[r, u], fs.at[u, r], fr.at[u, r], dev(0, 0, 0, r)))
    for u in range(2):
        total = f_own[u]
        for r in (1, 3, 2):
            copy(f_out.at[r, u], f_in.at[r, u], fs.at[u, r], fr.at[u, r], partner).wait_recv()
            total = total + f_in[r, u].astype(F32)
        f_all[z, u] = total.astype(BF)
        for r in (2, 1, 3):
            go(copy(f_all.at[z, u], f_all.at[z, u], gs.at[u, r], gr.at[u, r], dev(0, 0, 0, r)))

    gram = jnp.zeros((64, 128), F32)
    for u in range(2):
        mat = f_all[z, u]
        gram = gram + dot_nt(mat, jnp.concatenate([mat, mat], axis=0))
    lane, row = iota((32, 128), 1), iota((32, 128), 0)
    eye = jnp.where(lane % 32 == row, 1.0, 0.0)
    work = jnp.where(lane >= 96, gram[32:64], jnp.where(lane >= 64, gram[0:32], eye))
    first = (lane // 32) % 2 == 0
    for k in range(32):
        one = work[:, 64 + k : 65 + k]
        two = work[:, 96 + k : 97 + k]
        factor = jnp.where(first, one / one[k : k + 1, :], two / two[k : k + 1, :])
        factor = jnp.where(row > k, factor, 0.0)
        work = work - factor * work[k : k + 1, :]
    one = jnp.sum(jnp.where(lane == 64 + row, work, 0.0), axis=1, keepdims=True)
    two = jnp.sum(jnp.where(lane == 96 + row, work, 0.0), axis=1, keepdims=True)
    low[z] = work * jnp.where(first, 1.0 / jnp.sqrt(one), 1.0 / jnp.sqrt(two))
    for r in (2, 1, 3):
        go(copy(low.at[z], low.at[z], ls.at[r], lr.at[r], dev(0, 0, 0, r)))

    for u in range(2):
        for r in (0, 1, 3, 2):
            zz = turn(z, 4 - r)
            if r:
                copy(f_all.at[zz, u], f_all.at[zz, u], gs.at[u, r], gr.at[u, r], partner).wait_recv()
            for i in range(2):
                j = zz * 2 + i
                at = pl.ds(pl.multiple_of(j * 32, 32), 32)
                got = dot_nt(f_all[zz, u, i * 32 : i * 32 + 32, :], hid[j, :, u * units : u * units + units])
                hf[at, :] = hf[at, :] + got if u else got
    place64 = iota((32, 64), 1) < 32

    def lower(zz):
        both = low[zz][:, 0:64]
        return jnp.concatenate([jnp.where(place64, both, 0.0), jnp.where(place64, 0.0, both)], axis=0)

    for r in (0, 1, 3, 2):
        zz = turn(z, 4 - r)
        if r:
            copy(low.at[zz], low.at[zz], ls.at[r], lr.at[r], partner).wait_recv()
        at = pl.ds(pl.multiple_of(zz * 64, 64), 64)
        m_t[at, :] = dot_nn(lower(zz), hf[at, :], precision=HI).astype(BF)
    while waits:
        waits.pop(0).wait_send()
    while waits:
        waits.pop(0).wait_send()
    for h in range(2):
        spreads = dot_nt(select[h], m_t[...]).astype(BF)
        for r in range(4):
            m_out[h, 0, r] = spreads[r * 64 : r * 64 + 64]
        p_in[h, 0, z] = spreads[0:64]
        for r in (2, 1, 3, 0):
            for q in (2, 1, 3, 0):
                if r or q:
                    go(
                        copy(
                            m_out.at[h, 0, r], p_in.at[h, r, z], js.at[h, r, q], jr.at[h, r, q],
                            dev(h, 0, 4 - r, q),
                        )
                    )
    for zz in range(4):
        mat = lower(zz)
        top = mat.astype(BF)
        rest = (mat - top.astype(F32)).astype(BF)
        for u in range(2):
            both = dot_nn(top, f_all[zz, u]) + dot_nn(rest, f_all[zz, u])
            basis_ref[zz * 64 : zz * 64 + 64, u * units : u * units + units] = both.astype(BF)

    for r in (2, 1, 3, 0):
        for h in range(2):
            b = turn(spread[h], r)
            for q in range(4):
                if r or q:
                    zz = turn(z, 4 - q)
                    copy(m_out.at[h, 0, r], p_in.at[h, r, zz], js.at[h, r, q], jr.at[h, r, q], partner).wait_recv()
            terms = jnp.concatenate([p_in[h, r, zz] for zz in range(4)], axis=0)
            p_t[...] = terms.astype(F32).T.astype(BF)

            @pl.loop(0, 8)
            def _(j):
                at = pl.ds(pl.multiple_of(j * 32, 32), 32)
                got = dot_nn(p_t[at, :], routed[h, b * 8 + j])
                if r:
                    to = pl.ds(pl.multiple_of((j % 4) * 32, 32), 32)
                    tok[h, 2 * r + j // 4, to, :] = got.astype(BF)
                else:
                    update_ref[at, h * width : h * width + width] = got

            if r:
                go(
                    copy(
                        tok.at[h, pl.ds(2 * r, 2)], tok.at[h, pl.ds(8 + 2 * r, 2)], us.at[h, r], ur.at[h, r],
                        dev(h, 0, r, 0),
                    )
                )
    for r in (1, 3, 2):
        for h in range(2):
            copy(
                tok.at[h, pl.ds(2 * r, 2)], tok.at[h, pl.ds(8 + 2 * r, 2)], us.at[h, r], ur.at[h, r], partner
            ).wait_recv()

            @pl.loop(0, 8)
            def _(j):
                at = pl.ds(pl.multiple_of(j * 32, 32), 32)
                to = pl.ds(pl.multiple_of((j % 4) * 32, 32), 32)
                side = slice(h * width, h * width + width)
                update_ref[at, side] = update_ref[at, side] + tok[h, 8 + 2 * r + j // 4, to, :].astype(F32)

    for cp in waits:
        cp.wait_send()


def local(out_grads, expert_ids, gate_probs, hidden_acts, q_previous):
    experts, rank, model = q_previous.shape
    hidden_units = hidden_acts.shape[3]
    width = model // lax.axis_size("dp")
    half = width // 2
    any_spec, vmem = pl.BlockSpec(memory_space=pl.ANY), pl.BlockSpec(memory_space=pltpu.VMEM)
    dma = lambda *shape: pltpu.SemaphoreType.DMA(shape)
    basis, update = pl.pallas_call(
        kernel,
        out_shape=(
            jax.ShapeDtypeStruct((experts * rank, hidden_units), BF),
            jax.ShapeDtypeStruct((experts * rank, width), F32),
        ),
        in_specs=[vmem, vmem, any_spec, any_spec, any_spec],
        out_specs=(vmem, vmem),
        scratch_shapes=[
            pltpu.VMEM((2, 32, 128, half), BF),
            pltpu.VMEM((2, 32, 16, 128), F32),
            pltpu.VMEM((2, 4, 256, half), BF),
            pltpu.VMEM((2, 32, 256, half), BF),
            pltpu.VMEM((8, 192, hidden_units), BF),
            pltpu.VMEM((2, 4, 4, 64, 256), BF),
            pltpu.VMEM((2, 4, 4, 64, 256), BF),
            pltpu.VMEM((256, 192), BF),
            pltpu.VMEM((256, 192), F32),
            pltpu.VMEM((4, 2, 64, hidden_units // 2), BF),
            pltpu.VMEM((4, 2, 64, hidden_units // 2), BF),
            pltpu.VMEM((2, 64, hidden_units // 2), F32),
            pltpu.VMEM((4, 2, 64, hidden_units // 2), BF),
            pltpu.VMEM((4, 32, 128), F32),
            pltpu.VMEM((2, 4, 4, 64, 256), BF),
            pltpu.VMEM((256, 256), BF),
            dma(5),
            dma(2, 4), dma(2, 4), dma(2, 2, 4), dma(2, 2, 4), dma(2, 2, 4), dma(2, 2, 4), dma(2, 4, 4), dma(2, 4, 4),
            dma(2, 4), dma(2, 4), dma(2, 2, 4), dma(2, 2, 4), dma(2, 4), dma(2, 4), dma(2, 4, 4), dma(2, 4, 4),
            dma(2, 4), dma(2, 4), dma(2, 4, 4), dma(2, 4, 4), dma(2, 4), dma(2, 4), dma(2, 4), dma(2, 4), dma(4), dma(4),
            dma(2, 4, 4), dma(2, 4, 4), dma(2, 4), dma(2, 4),
        ],
        compiler_params=pltpu.CompilerParams(
            collective_id=0, has_side_effects=True, vmem_limit_bytes=67043328
        ),
    )(
        expert_ids[0].T,
        gate_probs[0].T,
        out_grads[0],
        hidden_acts[0],
        q_previous.reshape(experts * rank, model),
    )
    basis = basis.reshape(experts, rank, hidden_units).astype(F32) * math.sqrt(hidden_units)
    return (basis, update.reshape(experts, rank, width))


def solution(mesh):
    return jax.shard_map(
        local,
        mesh=mesh,
        in_specs=(
            P("dp", "expert", None),
            P("dp", "expert", None),
            P("dp", "expert", None),
            P("dp", "expert", None, None),
            P("expert", None, None),
        ),
        out_specs=(P("expert", None, None), P("expert", None, "dp")),
        check_vma=False,
    )
```

```python
import math

import jax
import jax.numpy as jnp
from jax import lax
from jax.experimental import pallas as pl
from jax.experimental.pallas import tpu as pltpu
from jax.sharding import PartitionSpec as P

MESH = pl.DeviceIdType.MESH
BF, F32 = jnp.bfloat16, jnp.float32
HI = lax.Precision.HIGHEST
SLOT = 8
CAP = 6


def dot_nt(left, right, **more):
    return lax.dot_general(left, right, (((1,), (1,)), ((), ())), preferred_element_type=F32, **more)


def dot_nn(left, right, **more):
    return lax.dot_general(left, right, (((1,), (0,)), ((), ())), preferred_element_type=F32, **more)


def dot_tn(left, right, **more):
    return lax.dot_general(left, right, (((0,), (0,)), ((), ())), preferred_element_type=F32, **more)


def iota(shape, dim):
    return lax.broadcasted_iota(jnp.int32, shape, dim)


def kernel(
    ids_ref, gates_ref, grads_ref, hidden_ref, prev_ref, basis_ref, update_ref,
    tok, meta, q_row, routed, hid, m_out, m_in, m_t, hf, f_out, f_in, f_own, f_all, low, p_in, p_t,
    load_sem, zs, zr, as_, ar, hs, hr, ps, pr,
    mzs, mzr, mas, mar, mhs, mhr, mps, mpr,
    qs, qr, ms, mr, fs, fr, gs, gr, ls, lr, js, jr, us, ur,
):
    width = tok.shape[3]
    e, z = lax.axis_index("expert"), lax.axis_index("dp")
    y, x, c = e // 8, (e // 2) % 4, e % 2
    gather, spread = (y, x), (x, y)

    def turn(v, by):
        return lax.rem(v + by, 4)

    def dev(h, along_gather, along_spread, to_z, core=0):
        g, s = turn(gather[h], along_gather), turn(spread[h], along_spread)
        yy, xx = (g, s) if h == 0 else (s, g)
        cc = 1 - c if core else c
        return {"expert": (yy * 4 + xx) * 2 + cc, "dp": turn(z, to_z)}

    def copy(src, dst, send, recv, device):
        return pltpu.make_async_remote_copy(src, dst, send, recv, device_id=device, device_id_type=MESH)

    def block(zz, gg, cc):
        return (zz * 4 + gg) * 2 + cc

    def cols(zz, h):
        return pl.ds(pl.multiple_of(zz * (2 * width) + h * width, 128), width)

    own = [block(z, gather[h], c) for h in range(2)]
    load_tok = [
        pltpu.make_async_copy(grads_ref.at[:, cols(z, h)], tok.at[h, own[h]], load_sem.at[h])
        for h in range(2)
    ]
    load_q = [
        pltpu.make_async_copy(prev_ref.at[:, cols(z, h)], q_row.at[h, spread[h]], load_sem.at[2 + h])
        for h in range(2)
    ]
    load_hid = pltpu.make_async_copy(hidden_ref, hid, load_sem.at[4])
    for cp in load_tok + load_q + [load_hid]:
        cp.start()

    barrier = pltpu.get_barrier_semaphore()
    peers = [dev(0, 0, 0, 0, core=1)] + [dev(0, 0, 0, r) for r in (1, 2, 3)]
    for h in range(2):
        for b in (1, 2, 3):
            for r in range(4):
                peers.append(dev(h, 0, b, r))
    for peer in peers:
        pl.semaphore_signal(barrier, inc=1, device_id=peer, device_id_type=MESH)

    ids = ids_ref[...]
    expert_row = iota((256, 128), 0)
    named = jnp.zeros((256, 128), F32)
    for k in range(8):
        named = named + jnp.where(ids[k : k + 1, :] == expert_row, 1.0, 0.0)
    before = jnp.where(iota((128, 128), 0) < iota((128, 128), 1), 1.0, 0.0).astype(BF)
    earlier = dot_nn(named.astype(BF), before)
    place = jnp.concatenate(
        [
            jnp.sum(jnp.where(ids[k : k + 1, :] == expert_row, earlier, 0.0), axis=0, keepdims=True)
            for k in range(8)
        ],
        axis=0,
    )
    holder, inner = ids // 8, ids % 8
    at_y, at_x, at_c = holder // 8, (holder // 2) % 4, holder % 2
    for h, (g, s) in enumerate(((at_y, at_x), (at_x, at_y))):
        base = (g * 2 + at_c) * 256 + (s * 8 + inner) * SLOT
        meta[h, own[h], 0:8, :] = base.astype(F32) + place
        meta[h, own[h], 8:16, :] = gates_ref[...]

    pl.semaphore_wait(barrier, len(peers))

    waits = []

    def go(cp):
        cp.start()
        waits.append(cp)

    zorder = [1, 3, 2, 0]
    for h in range(2):
        load_q[h].wait()
        b = spread[h]
        for way in range(2):
            go(copy(q_row.at[h, b], q_row.at[h, b], qs.at[h, way], qr.at[h, way], dev(h, 0, 1 + 2 * way, 0)))
    for r in (1, 3, 2):
        for h in range(2):
            b = own[h]
            to = turn(z, r)
            go(copy(meta.at[h, b], meta.at[h, b], mzs.at[h, r], mzr.at[h, r], dev(0, 0, 0, r)))
            go(copy(grads_ref.at[:, cols(to, h)], tok.at[h, b], zs.at[h, r], zr.at[h, r], dev(0, 0, 0, r)))

    partner = dev(0, 0, 0, 0, core=1)

    def to_partner(h, k, zz, dg):
        b = block(zz, turn(gather[h], dg), c)
        go(copy(meta.at[h, b], meta.at[h, b], mps.at[h, k, dg], mpr.at[h, k, dg], partner))
        go(copy(tok.at[h, b], tok.at[h, b], ps.at[h, k, dg], pr.at[h, k, dg], partner))

    def source(k):
        return turn(z, zorder[k])

    def stage_a(k):
        zz = source(k)
        for h in range(2):
            b = block(zz, gather[h], c)
            if zorder[k]:
                r = (4 - zorder[k]) % 4
                copy(meta.at[h, b], meta.at[h, b], mzs.at[h, r], mzr.at[h, r], partner).wait_recv()
                copy(tok.at[h, b], tok.at[h, b], zs.at[h, r], zr.at[h, r], partner).wait_recv()
            else:
                load_tok[h].wait()
            for way, step in ((0, 1), (1, 3)):
                device = dev(h, step, 0, 0)
                go(copy(meta.at[h, b], meta.at[h, b], mas.at[h, way, k], mar.at[h, way, k], device))
                go(copy(tok.at[h, b], tok.at[h, b], as_.at[h, way, k], ar.at[h, way, k], device))
            to_partner(h, k, zz, 0)

    def stage_b(k):
        zz = source(k)
        for h in range(2):
            for way, step, dg in ((0, 1, 3), (1, 3, 1)):
                device = dev(h, step, 0, 0)
                b = block(zz, turn(gather[h], dg), c)
                copy(meta.at[h, b], meta.at[h, b], mas.at[h, way, k], mar.at[h, way, k], device).wait_recv()
                copy(tok.at[h, b], tok.at[h, b], as_.at[h, way, k], ar.at[h, way, k], device).wait_recv()
                half = pl.ds(way * 64, 64)
                if way == 0:
                    go(copy(meta.at[h, b], meta.at[h, b], mhs.at[h, k], mhr.at[h, k], device))
                go(copy(tok.at[h, b, half], tok.at[h, b, half], hs.at[h, way, k], hr.at[h, way, k], device))
                to_partner(h, k, zz, dg)

    def stage_h(k):
        zz = source(k)
        for h in range(2):
            b = block(zz, turn(gather[h], 2), c)
            copy(meta.at[h, b], meta.at[h, b], mhs.at[h, k], mhr.at[h, k], partner).wait_recv()
            for way in range(2):
                half = pl.ds(way * 64, 64)
                copy(
                    tok.at[h, b, half], tok.at[h, b, half], hs.at[h, way, k], hr.at[h, way, k], partner
                ).wait_recv()
            to_partner(h, k, zz, 2)

    mine = [((gather[h] * 2 + c) * 256).astype(F32) for h in range(2)]
    row_of = iota((256, 128), 0).astype(F32)
    chunks = [(n, min(256, width - n)) for n in range(0, width, 256)]

    def rows_of(h, zz, gg):
        pair = zz * 4 + gg
        less = jnp.where(h == 0, mine[0], mine[1])
        picks, scales = [], []
        for cc in range(2):
            info = meta[h, pair * 2 + cc]
            want = info[0:8] - less
            gate = jnp.zeros((256, 128), F32)
            for k in range(8):
                gate = jnp.where(row_of == want[k : k + 1], info[8 + k : 9 + k], gate)
            picks.append(jnp.where(gate > 0.0, 1.0, 0.0).astype(BF))
            scales.append(jnp.sum(gate, axis=1, keepdims=True))
        to = pl.ds(pl.multiple_of(pair * 16, 16), 16)
        for n, size in chunks:
            got = [
                (dot_nn(picks[cc], tok[h, pair * 2 + cc, :, n : n + size]) * scales[cc]).reshape(32, 8, size)
                for cc in range(2)
            ]
            routed[h, :, to, n : n + size] = jnp.concatenate(got, axis=1).astype(BF)

    lane_expert = iota((64, 256), 1) // 32

    def wait_partner(k, dg):
        zz = source(k)
        for h in range(2):
            b = block(zz, turn(gather[h], dg), 1 - c)
            copy(meta.at[h, b], meta.at[h, b], mps.at[h, k, dg], mpr.at[h, k, dg], partner).wait_recv()
            copy(tok.at[h, b], tok.at[h, b], ps.at[h, k, dg], pr.at[h, k, dg], partner).wait_recv()

    def stage_rows(k):
        zz = source(k)
        for dg in (0, 1, 3):
            wait_partner(k, dg)

        @pl.loop(0, 6)
        def _(i):
            h, n = i % 2, i // 2
            rows_of(h, zz, turn(jnp.where(h == 0, y, x), n + n // 2))

        wait_partner(k, 2)

        @pl.loop(0, 2)
        def _(h):
            rows_of(h, zz, turn(jnp.where(h == 0, y, x), 2))

    def stage_mix(k):
        zz = source(k)
        part = pl.ds(pl.multiple_of(zz * 64, 64), 64)
        for h in range(2):
            for r in (2, 1, 3, 0):
                to = turn(spread[h], r)
                rows = routed[h, pl.ds(to * 8, 8), part, :].reshape(512, width)
                every = dot_nt(rows, q_row[h, to])
                total = jnp.zeros((64, 256), F32)
                for j in range(8):
                    total = total + jnp.where(lane_expert == j, every[j * 64 : j * 64 + 64], 0.0)
                if zorder[k] == 0 and r == 0:
                    m_in[h, 0, k] = total.astype(BF)
                else:
                    m_out[h, k, r] = total.astype(BF)
                    go(
                        copy(
                            m_out.at[h, k, r], m_in.at[h, r, k], ms.at[h, k, r], mr.at[h, k, r],
                            dev(h, 0, r, zorder[k]),
                        )
                    )

    for h in range(2):
        for way, back in ((0, 3), (1, 1)):
            b = turn(spread[h], back)
            copy(q_row.at[h, b], q_row.at[h, b], qs.at[h, way], qr.at[h, way], partner).wait_recv()
            part = pl.ds(way * 128, 128)
            go(
                copy(
                    q_row.at[h, b, part], q_row.at[h, b, part], qs.at[h, 2 + way], qr.at[h, 2 + way],
                    dev(h, 0, 1 + 2 * way, 0),
                )
            )
    stage_a(0)
    stage_a(1)
    stage_b(0)
    stage_a(2)
    stage_h(0)
    stage_b(1)
    stage_a(3)
    stage_rows(0)
    stage_h(1)
    stage_b(2)
    for h in range(2):
        b = turn(spread[h], 2)
        for way in range(2):
            part = pl.ds(way * 128, 128)
            copy(
                q_row.at[h, b, part], q_row.at[h, b, part], qs.at[h, 2 + way], qr.at[h, 2 + way], partner
            ).wait_recv()
    stage_mix(0)
    stage_rows(1)
    stage_h(2)
    stage_b(3)
    stage_mix(1)
    stage_rows(2)
    stage_h(3)
    stage_mix(2)
    stage_rows(3)
    stage_mix(3)

    while waits:
        waits.pop(0).wait_send()

    load_hid.wait()

    def selection(h):
        row, slot = iota((256, 192), 0), iota((256, 192), 1)
        back = turn(spread[h] + 4 - row // 64, 0)
        along = (row // 16) % 4
        yy, xx = (along, back) if h == 0 else (back, along)
        at = ((yy * 4 + xx) * 2 + (row // 8) % 2) * CAP + row % 8
        return jnp.where((at == slot) & (row % 8 < CAP), 1.0, 0.0).astype(BF)

    select = [selection(h) for h in range(2)]
    mixed = jnp.zeros((256, 192), F32)
    for h in range(2):
        parts = []
        for r in range(4):
            total = None
            for k in range(4):
                if zorder[k] or r:
                    copy(
                        m_out.at[h, k, r], m_in.at[h, r, k], ms.at[h, k, r], mr.at[h, k, r], partner
                    ).wait_recv()
                got = m_in[h, r, k].astype(F32)
                total = got if total is None else total + got
            parts.append(total)
        raw = jnp.concatenate(parts, axis=0)
        top = raw.astype(BF)
        rest = (raw - top.astype(F32)).astype(BF)
        mixed = mixed + dot_tn(top, select[h]) + dot_tn(rest, select[h])
    m_t[...] = mixed.astype(BF)

    units = hid.shape[2] // 4
    for u in range(4):
        for r in (2, 1, 3, 0):
            to = turn(z, r)
            for i in range(2):
                j = to * 2 + i
                rows = m_t[pl.ds(pl.multiple_of(j * 32, 32), 32), :]
                got = dot_nn(rows, hid[j, :, u * units : u * units + units])
                if r:
                    f_out[r, u, i * 32 : i * 32 + 32, :] = got.astype(BF)
                else:
                    f_own[u, i * 32 : i * 32 + 32, :] = got
            if r:
                go(copy(f_out.at[r, u], f_in.at[r, u], fs.at[u, r], fr.at[u, r], dev(0, 0, 0, r)))
    for u in range(4):
        total = f_own[u]
        for r in (1, 3, 2):
            copy(f_out.at[r, u], f_in.at[r, u], fs.at[u, r], fr.at[u, r], partner).wait_recv()
            total = total + f_in[r, u].astype(F32)
        f_all[z, u] = total.astype(BF)
        for r in (2, 1, 3):
            go(copy(f_all.at[z, u], f_all.at[z, u], gs.at[u, r], gr.at[u, r], dev(0, 0, 0, r)))

    gram = jnp.zeros((64, 128), F32)
    for u in range(4):
        mat = f_all[z, u]
        gram = gram + dot_nt(mat, jnp.concatenate([mat, mat], axis=0))
    lane, row = iota((32, 128), 1), iota((32, 128), 0)
    eye = jnp.where(lane % 32 == row, 1.0, 0.0)
    work = jnp.where(lane >= 96, gram[32:64], jnp.where(lane >= 64, gram[0:32], eye))
    first = (lane // 32) % 2 == 0
    for k in range(32):
        one = work[:, 64 + k : 65 + k]
        two = work[:, 96 + k : 97 + k]
        factor = jnp.where(first, one / one[k : k + 1, :], two / two[k : k + 1, :])
        factor = jnp.where(row > k, factor, 0.0)
        work = work - factor * work[k : k + 1, :]
    one = jnp.sum(jnp.where(lane == 64 + row, work, 0.0), axis=1, keepdims=True)
    two = jnp.sum(jnp.where(lane == 96 + row, work, 0.0), axis=1, keepdims=True)
    low[z] = work * jnp.where(first, 1.0 / jnp.sqrt(one), 1.0 / jnp.sqrt(two))
    for r in (2, 1, 3):
        go(copy(low.at[z], low.at[z], ls.at[r], lr.at[r], dev(0, 0, 0, r)))

    for u in range(4):
        for r in (0, 1, 3, 2):
            zz = turn(z, 4 - r)
            if r:
                copy(f_all.at[zz, u], f_all.at[zz, u], gs.at[u, r], gr.at[u, r], partner).wait_recv()
            for i in range(2):
                j = zz * 2 + i
                at = pl.ds(pl.multiple_of(j * 32, 32), 32)
                got = dot_nt(f_all[zz, u, i * 32 : i * 32 + 32, :], hid[j, :, u * units : u * units + units])
                hf[at, :] = hf[at, :] + got if u else got
    place64 = iota((32, 64), 1) < 32

    def lower(zz):
        both = low[zz][:, 0:64]
        return jnp.concatenate([jnp.where(place64, both, 0.0), jnp.where(place64, 0.0, both)], axis=0)

    for r in (0, 1, 3, 2):
        zz = turn(z, 4 - r)
        if r:
            copy(low.at[zz], low.at[zz], ls.at[r], lr.at[r], partner).wait_recv()
        at = pl.ds(pl.multiple_of(zz * 64, 64), 64)
        m_t[at, :] = dot_nn(lower(zz), hf[at, :], precision=HI).astype(BF)
    while waits:
        waits.pop(0).wait_send()
    while waits:
        waits.pop(0).wait_send()
    for h in range(2):
        spreads = dot_nt(select[h], m_t[...]).astype(BF)
        for r in range(4):
            m_out[h, 0, r] = spreads[r * 64 : r * 64 + 64]
        p_in[h, 0, z] = spreads[0:64]
        for r in (2, 1, 3, 0):
            for q in (2, 1, 3, 0):
                if r or q:
                    go(
                        copy(
                            m_out.at[h, 0, r], p_in.at[h, r, z], js.at[h, r, q], jr.at[h, r, q],
                            dev(h, 0, 4 - r, q),
                        )
                    )
    for zz in range(4):
        mat = lower(zz)
        top = mat.astype(BF)
        rest = (mat - top.astype(F32)).astype(BF)
        for u in range(4):
            both = dot_nn(top, f_all[zz, u]) + dot_nn(rest, f_all[zz, u])
            basis_ref[zz * 64 : zz * 64 + 64, u * units : u * units + units] = both.astype(BF)

    for r in (2, 1, 3, 0):
        for h in range(2):
            b = turn(spread[h], r)
            for q in range(4):
                if r or q:
                    zz = turn(z, 4 - q)
                    copy(m_out.at[h, 0, r], p_in.at[h, r, zz], js.at[h, r, q], jr.at[h, r, q], partner).wait_recv()
            terms = jnp.concatenate([p_in[h, r, zz] for zz in range(4)], axis=0)
            p_t[...] = terms.astype(F32).T.astype(BF)

            @pl.loop(0, 8)
            def _(j):
                at = pl.ds(pl.multiple_of(j * 32, 32), 32)
                got = dot_nn(p_t[at, :], routed[h, b * 8 + j])
                if r:
                    to = pl.ds(pl.multiple_of((j % 4) * 32, 32), 32)
                    tok[h, 2 * r + j // 4, to, :] = got.astype(BF)
                else:
                    update_ref[at, h * width : h * width + width] = got

            if r:
                go(
                    copy(
                        tok.at[h, pl.ds(2 * r, 2)], tok.at[h, pl.ds(8 + 2 * r, 2)], us.at[h, r], ur.at[h, r],
                        dev(h, 0, r, 0),
                    )
                )
    for r in (1, 3, 2):
        for h in range(2):
            copy(
                tok.at[h, pl.ds(2 * r, 2)], tok.at[h, pl.ds(8 + 2 * r, 2)], us.at[h, r], ur.at[h, r], partner
            ).wait_recv()

            @pl.loop(0, 8)
            def _(j):
                at = pl.ds(pl.multiple_of(j * 32, 32), 32)
                to = pl.ds(pl.multiple_of((j % 4) * 32, 32), 32)
                side = slice(h * width, h * width + width)
                update_ref[at, side] = update_ref[at, side] + tok[h, 8 + 2 * r + j // 4, to, :].astype(F32)

    for cp in waits:
        cp.wait_send()


def local(out_grads, expert_ids, gate_probs, hidden_acts, q_previous):
    experts, rank, model = q_previous.shape
    hidden_units = hidden_acts.shape[3]
    width = model // lax.axis_size("dp")
    half = width // 2
    any_spec, vmem = pl.BlockSpec(memory_space=pl.ANY), pl.BlockSpec(memory_space=pltpu.VMEM)
    dma = lambda *shape: pltpu.SemaphoreType.DMA(shape)
    basis, update = pl.pallas_call(
        kernel,
        out_shape=(
            jax.ShapeDtypeStruct((experts * rank, hidden_units), BF),
            jax.ShapeDtypeStruct((experts * rank, width), F32),
        ),
        in_specs=[vmem, vmem, any_spec, any_spec, any_spec],
        out_specs=(vmem, vmem),
        scratch_shapes=[
            pltpu.VMEM((2, 32, 128, half), BF),
            pltpu.VMEM((2, 32, 16, 128), F32),
            pltpu.VMEM((2, 4, 256, half), BF),
            pltpu.VMEM((2, 32, 256, half), BF),
            pltpu.VMEM((8, 192, hidden_units), BF),
            pltpu.VMEM((2, 4, 4, 64, 256), BF),
            pltpu.VMEM((2, 4, 4, 64, 256), BF),
            pltpu.VMEM((256, 192), BF),
            pltpu.VMEM((256, 192), F32),
            pltpu.VMEM((4, 4, 64, hidden_units // 4), BF),
            pltpu.VMEM((4, 4, 64, hidden_units // 4), BF),
            pltpu.VMEM((4, 64, hidden_units // 4), F32),
            pltpu.VMEM((4, 4, 64, hidden_units // 4), BF),
            pltpu.VMEM((4, 32, 128), F32),
            pltpu.VMEM((2, 4, 4, 64, 256), BF),
            pltpu.VMEM((256, 256), BF),
            dma(5),
            dma(2, 4), dma(2, 4), dma(2, 2, 4), dma(2, 2, 4), dma(2, 2, 4), dma(2, 2, 4), dma(2, 4, 4), dma(2, 4, 4),
            dma(2, 4), dma(2, 4), dma(2, 2, 4), dma(2, 2, 4), dma(2, 4), dma(2, 4), dma(2, 4, 4), dma(2, 4, 4),
            dma(2, 4), dma(2, 4), dma(2, 4, 4), dma(2, 4, 4), dma(4, 4), dma(4, 4), dma(4, 4), dma(4, 4), dma(4), dma(4),
            dma(2, 4, 4), dma(2, 4, 4), dma(2, 4), dma(2, 4),
        ],
        compiler_params=pltpu.CompilerParams(
            collective_id=0, has_side_effects=True, vmem_limit_bytes=67043328
        ),
    )(
        expert_ids[0].T,
        gate_probs[0].T,
        out_grads[0],
        hidden_acts[0],
        q_previous.reshape(experts * rank, model),
    )
    basis = basis.reshape(experts, rank, hidden_units).astype(F32) * math.sqrt(hidden_units)
    return (basis, update.reshape(experts, rank, width))


def solution(mesh):
    return jax.shard_map(
        local,
        mesh=mesh,
        in_specs=(
            P("dp", "expert", None),
            P("dp", "expert", None),
            P("dp", "expert", None),
            P("dp", "expert", None, None),
            P("expert", None, None),
        ),
        out_specs=(P("expert", None, None), P("expert", None, "dp")),
        check_vma=False,
    )
```
